32 devices in a mesh: view: 4 (over x, core), gz: 8 (over z, y).
Axes of the slice: x: 2, y: 2, z: 4, core: 2. Of those that a mesh axis runs over, the one named last changes fastest.
Arguments:
- views_data: float32 [4, 128, 128, 384], P('view', 'gz'), may hold values from 0.25 to 4
- start: float32 [128, 128, 384], P('gz'), may hold values from 0.5 to 2
- psf_table: float32 [8, 3, 17], replicated, may hold values from 0.05 to 1
- psf_index: int32 [4], P('view'), may hold values from 0 to 7
Outputs:
- estimate: float32 [128, 128, 384], P('gz')
The draws below stay inside these ranges and needn't reach their ends.
All inputs are finite; a program needn't handle non-finite values.
Results may differ from the reference program's by a relative error of at most 0.0001.
Values sent between devices are 32-bit elements; how exact they have to be, the bound alone decides.
A program may use at most 128 MiB of HBM per device.

```python
import math
import jax
import jax.numpy as jnp
from jax import lax

NX = 128
NY = 384
RAD = 8
ITERS = 2
NPSF = 8
VIEWS = 4
TAPS = 17
NZ = 128


def plant(result, rng, least, high):
    extent = result.shape
    place = [jax.random.randint(jax.random.fold_in(rng, axis), (), 0, extent[axis]) for axis in range(len(extent))]
    result = result.at[tuple(place)].set(least)
    longest = extent.index(max(extent))
    place[longest] = (place[longest] + 1) % extent[longest]
    return result.at[tuple(place)].set(high)


def level_of(stream_key, shape, shards, smallest, high):
    def one(position, shards_of):
        steps = jax.random.uniform(jax.random.fold_in(jax.random.fold_in(stream_key, 6), position), (shards_of,), jnp.float32, smallest / len(shards), high / len(shards))
        return jnp.repeat(jnp.exp(steps), shape[position] // shards_of).reshape((-1,) + (1,) * (len(shape) - position - 1))

    gain = one(*shards[0])
    for cut in shards[1:]:
        gain = gain * one(*cut)
    return gain


def setup_inputs(seed: int = 0) -> dict:
    arg_keys = jax.random.split(jax.random.key(seed), 5)
    return {
        "views_data": jnp.clip(jnp.exp(math.log(4.0) - 2.7725887 * jax.random.uniform(arg_keys[0], (VIEWS, NZ, NX, NY), jnp.float32) ** level_of(arg_keys[0], (VIEWS, NZ, NX, NY), ((0, 4), (1, 8)), -0.2, 0.2)), 0.25, 4.0),
        "start": jnp.clip(jnp.exp(math.log(2.0) - 1.3862944 * jax.random.uniform(arg_keys[1], (NZ, NX, NY), jnp.float32) ** level_of(arg_keys[1], (NZ, NX, NY), ((0, 8),), -0.2, 0.2)), 0.5, 2.0),
        "psf_table": jnp.clip(jnp.exp(jax.random.uniform(arg_keys[2], (NPSF, 3, TAPS), jnp.float32, math.log(0.05), math.log(1.0))), 0.05, 1.0),
        "psf_index": plant(jax.random.randint(arg_keys[3], (VIEWS,), 0, NPSF), jax.random.fold_in(arg_keys[3], 1), 0, NPSF - 1).astype(jnp.int32),
    }


def band_matrix(kern_row, length):
    places = jnp.arange(length)
    offsets = places[None, :] - places[:, None]
    tap_shift = jnp.arange(2 * RAD + 1) - RAD
    matches = (offsets[None, :, :] == tap_shift[:, None, None]).astype(jnp.float32)
    return jnp.sum(kern_row[:, None, None] * matches, axis=0)


def blur_planes(volume, mat_x, mat_y):
    along_x = jnp.einsum("ij,zjy->ziy", mat_x, volume, precision=lax.Precision.HIGHEST)
    return jnp.einsum("zxj,ij->zxi", along_x, mat_y, precision=lax.Precision.HIGHEST)


def back_planes(volume, mat_x, mat_y):
    along_x = jnp.einsum("ij,ziy->zjy", mat_x, volume, precision=lax.Precision.HIGHEST)
    return jnp.einsum("zxi,ij->zxj", along_x, mat_y, precision=lax.Precision.HIGHEST)


def forward_z(padded, kern_z, rows):
    total = kern_z[0] * padded[0:rows]
    for tap in range(1, 2 * RAD + 1):
        total = total + kern_z[tap] * padded[tap:tap + rows]
    return total


def backward_z(padded, kern_z, rows):
    total = kern_z[0] * padded[2 * RAD:2 * RAD + rows]
    for tap in range(1, 2 * RAD + 1):
        total = total + kern_z[tap] * padded[2 * RAD - tap:2 * RAD - tap + rows]
    return total


def reference(views_data, start, psf_table, psf_index):
    estimate = start
    widths = ((RAD, RAD), (0, 0), (0, 0))
    for step in range(ITERS):
        total = None
        for which in range(VIEWS):
            kern = psf_table[psf_index[which]]
            kern = kern / jnp.sum(kern, axis=-1, keepdims=True)
            mat_x = band_matrix(kern[1], NX)
            mat_y = band_matrix(kern[2], NY)
            planes = blur_planes(estimate, mat_x, mat_y)
            blurred = forward_z(jnp.pad(planes, widths), kern[0], NZ)
            ratio = views_data[which] / blurred
            smeared = backward_z(jnp.pad(ratio, widths), kern[0], NZ)
            correction = back_planes(smeared, mat_x, mat_y)
            total = correction if total is None else total * correction
        estimate = estimate * jnp.power(total, 1.0 / VIEWS)
    return estimate
```

```python
import functools
import jax
import jax.numpy as jnp
from jax import lax
from jax.experimental import pallas as pl
from jax.experimental.pallas import tpu as pltpu
from jax.sharding import PartitionSpec as P

ITERS = 2
GROUP = 8
PLANES = 4
MESH = pl.DeviceIdType.MESH
VMEM = pl.BlockSpec(memory_space=pltpu.VMEM)
ANY = pl.BlockSpec(memory_space=pl.ANY)
MIB = 1024 * 1024


def split(value):
    high = value.astype(jnp.bfloat16)
    return high, (value - high.astype(jnp.float32)).astype(jnp.bfloat16)


def dot(lhs, rhs):
    return jnp.dot(lhs, rhs, preferred_element_type=jnp.float32)


def odd_stride(rows):
    return rows + 8 if (rows // 8) % 2 == 0 else rows


class Place:
    def __init__(self, blocks):
        view, gz = lax.axis_index("view"), lax.axis_index("gz")
        self.blocks = blocks
        self.a, self.c = view // 2, view % 2
        self.k, self.b = gz // 2, gz % 2
        self.strip = self.strip_of(self.a, self.b)

    @staticmethod
    def strip_of(a, b):
        return 2 * a + (a + b) % 2

    def device(self, a=None, c=None, k=None, b=None):
        a = self.a if a is None else a
        c = self.c if c is None else c
        k = self.k if k is None else k
        b = self.b if b is None else b
        return (2 * a + c, 2 * k + b)

    def of_strip(self, strip):
        return self.device(a=strip // 2, b=(strip % 2 + strip // 2) % 2)

    def partner(self):
        return self.device(c=1 - self.c)

    def others(self):
        a, b = self.a, self.b
        return ((a, 1 - b), (1 - a, b), (1 - a, 1 - b))


def remote(src, dst, sems, index, device):
    send, recv = sems
    return pltpu.make_async_remote_copy(
        src_ref=src, dst_ref=dst, send_sem=send.at[index], recv_sem=recv.at[index],
        device_id=device, device_id_type=MESH,
    )


def greet(here, along_z, along_strips, square):
    barrier = pltpu.get_barrier_semaphore()

    def signal(device):
        pl.semaphore_signal(barrier, inc=1, device_id=device, device_id_type=MESH)

    signal(here.partner())
    count = 1
    if square:
        for a, b in here.others():
            signal(here.device(a=a, b=b))
        count += 3
    around = []
    if along_z:
        around += [(here.k + step, here.blocks, lambda to: here.device(k=to)) for step in (-1, 1)]
    if along_strips:
        around += [(here.strip + step, 4, here.of_strip) for step in (-1, 1)]
    for there, limit, device in around:
        inside = (there >= 0) & (there < limit)
        pl.when(inside)(functools.partial(lambda there, device: signal(device(there)), there, device))
        count = count + inside.astype(jnp.int32)
    pl.semaphore_wait(barrier, count)


def band(taps, outputs, inputs, sign, shift):
    at = sign * (
        lax.broadcasted_iota(jnp.int32, (outputs, inputs), 1)
        - lax.broadcasted_iota(jnp.int32, (outputs, inputs), 0)
    ) + shift
    total = jnp.zeros((outputs, inputs), jnp.float32)
    for tap, value in enumerate(taps):
        total = jnp.where(at == tap, value, total)
    return total


def write_left(ref, index, matrix):
    high, low = split(matrix)
    rows, depth = matrix.shape
    top = jnp.concatenate([high, high], axis=1)
    bottom = jnp.concatenate([low, low], axis=1)
    ref[index] = jnp.concatenate([top, bottom], axis=0)


def write_right(ref, index, matrix):
    high, low = split(matrix)
    half = jnp.concatenate([high, low], axis=1)
    ref[index] = jnp.concatenate([half, half], axis=0)


def write_matrices(kern_ref, taps, refs):
    lz_ref, x_ref, ly_ref, lyb_ref, xb_ref, lzb_ref = refs
    reach = taps - 1
    pad = reach // 2
    for which in range(2):
        rows = kern_ref[which]
        kz, kx, ky = ([rows[r:r + 1, t:t + 1] for t in range(taps)] for r in range(3))
        outputs, inputs = lz_ref.shape[1] // 2, lz_ref.shape[2] // 2
        write_left(lz_ref, which, band(kz, outputs, inputs, 1, 0))
        write_right(x_ref, which, band(kx, x_ref.shape[1] // 2, x_ref.shape[2] // 2, -1, pad))
        write_left(ly_ref, which, band(ky, ly_ref.shape[1] // 2, ly_ref.shape[2] // 2, 1, 0))
        write_left(lyb_ref, which, band(ky, lyb_ref.shape[1] // 2, lyb_ref.shape[2] // 2, -1, reach))
        write_right(xb_ref, which, band(kx, xb_ref.shape[1] // 2, xb_ref.shape[2] // 2, 1, pad))
        write_left(lzb_ref, which, band(kz, lzb_ref.shape[1] // 2, lzb_ref.shape[2] // 2, -1, reach))


def setup_kernel(blocks, taps, strip_rows, data_hbm, start_hbm, kern_in,
                 est_ref, data_ref, lz_ref, x_ref, ly_ref, lyb_ref, xb_ref, lzb_ref,
                 sbuf, dbuf, ts_ref, td_ref, kern_ref,
                 load_sem, kern_s, kern_r, e_s, e_r, d_s, d_r, h_s, h_r):
    here = Place(blocks)
    planes, width_x, width_y = start_hbm.shape
    reach = taps - 1
    pad = reach // 2
    wide = strip_rows + 2 * reach
    tall = strip_rows + 2 * pad
    stride = ts_ref.shape[0] // (width_y + 2 * reach)
    half = wide // 2
    k, a, b, c = here.k, here.a, here.b, here.c
    load_start = pltpu.make_async_copy(start_hbm, sbuf, load_sem.at[0])
    load_data = pltpu.make_async_copy(data_hbm, dbuf, load_sem.at[1])
    load_start.start()
    load_data.start()
    ts3 = ts_ref.reshape(width_y + 2 * reach, stride, width_x)
    greet(here, True, False, True)

    kern_ref[a] = kern_in[...]
    kern_copy = remote(kern_in, kern_ref.at[a], (kern_s, kern_r), 0, here.device(a=1 - a))
    kern_copy.start()

    ts_ref[pl.ds(0, reach * stride)] = jnp.zeros((reach * stride, width_x), jnp.float32)
    ts_ref[pl.ds((width_y + reach) * stride, reach * stride)] = jnp.zeros((reach * stride, width_x), jnp.float32)
    load_start.wait()

    @pl.loop(0, planes)
    def _(z):
        ts_ref[pl.ds(reach * stride + z, width_y, stride=stride)] = sbuf[z].T

    mine = pl.multiple_of(reach + planes * b, planes)
    theirs = pl.multiple_of(reach + planes * (1 - b), planes)
    rows = pl.ds(half * c, half)
    to_strip = here.strip_of(a, 1 - b)
    e_copy = remote(
        ts3.at[pl.ds(strip_rows * to_strip + half * c, half), pl.ds(0, planes)],
        est_ref.at[rows, pl.ds(mine, planes)], (e_s, e_r), 0, here.device(b=1 - b),
    )
    e_copy.start()

    for z in range(planes):
        td_ref[z, pl.ds(0, pad)] = jnp.zeros((pad, width_x), jnp.float32)
        td_ref[z, pl.ds(pad + width_y, pad)] = jnp.zeros((pad, width_x), jnp.float32)
    load_data.wait()

    @pl.loop(0, planes)
    def _(z):
        td_ref[z, pl.ds(pad, width_y)] = dbuf[z].T

    edge = (b * (planes - pad), pad)
    inner = ((1 - b) * pad, planes - pad)
    d_copies = []
    for part, (first, size) in enumerate((edge, inner)):
        for kind, (oa, ob) in enumerate(here.others()):
            copy = remote(
                td_ref.at[pl.ds(first, size), pl.ds(strip_rows * here.strip_of(oa, ob), tall)],
                data_ref.at[a, pl.ds(pad + planes * b + first, size)],
                (d_s, d_r), 3 * part + kind, here.device(a=oa, b=ob),
            )
            copy.start()
            d_copies.append(copy)

    @pl.loop(0, wide)
    def _(row):
        est_ref[row, pl.ds(mine, planes)] = ts3[strip_rows * here.strip + row, pl.ds(0, planes)]

    @pl.loop(0, planes)
    def _(z):
        data_ref[a, pad + planes * b + z] = td_ref[z, pl.ds(pl.multiple_of(strip_rows * here.strip, 8), tall)]

    below, above = k > 0, k < blocks - 1

    def zero_est(first):
        @pl.loop(0, wide)
        def _(row):
            est_ref[row, pl.ds(first, reach)] = jnp.zeros((reach, width_x), jnp.float32)

    pl.when(jnp.logical_not(below))(lambda: zero_est(0))
    pl.when(jnp.logical_not(above))(lambda: zero_est(reach + 2 * planes))

    def halo(kind, oa, ob):
        to = k + 2 * ob - 1
        source = k + 1 - 2 * ob
        place = (1 - ob) * (2 * planes + pad)
        copy = remote(
            data_ref.at[oa, pl.ds(pad + ob * (2 * planes - pad), pad)],
            data_ref.at[oa, pl.ds(place, pad)],
            (h_s, h_r), kind, here.device(k=to),
        )
        sends = (to >= 0) & (to < blocks)
        gets = (source >= 0) & (source < blocks)

        @pl.when(jnp.logical_not(gets))
        def _():
            @pl.loop(0, pad)
            def _(z):
                data_ref[oa, place + z] = jnp.zeros((tall, width_x), jnp.float32)

        pl.when(sends)(copy.start)
        return copy, sends, gets

    halos = [halo(3, a, b)]

    kern_copy.wait()
    write_matrices(kern_ref, taps, (lz_ref, x_ref, ly_ref, lyb_ref, xb_ref, lzb_ref))

    e_copy.wait()
    relay = remote(
        est_ref.at[rows, pl.ds(theirs, planes)], est_ref.at[rows, pl.ds(theirs, planes)],
        (e_s, e_r), 1, here.partner(),
    )
    up = remote(
        est_ref.at[rows, pl.ds(2 * planes, reach)], est_ref.at[rows, pl.ds(0, reach)],
        (e_s, e_r), 2, here.device(k=k + 1),
    )
    down = remote(
        est_ref.at[rows, pl.ds(reach, reach)], est_ref.at[rows, pl.ds(reach + 2 * planes, reach)],
        (e_s, e_r), 3, here.device(k=k - 1),
    )
    pl.when(above)(up.start)
    pl.when(below)(down.start)
    relay.start()
    from_below = remote(
        est_ref.at[rows, pl.ds(0, reach)], est_ref.at[rows, pl.ds(0, reach)],
        (e_s, e_r), 4, here.partner(),
    )
    from_above = remote(
        est_ref.at[rows, pl.ds(reach + 2 * planes, reach)], est_ref.at[rows, pl.ds(reach + 2 * planes, reach)],
        (e_s, e_r), 5, here.partner(),
    )

    @pl.when(below)
    def _():
        up.wait_recv()
        from_below.start()

    @pl.when(above)
    def _():
        down.wait_recv()
        from_above.start()

    for kind, (oa, ob) in enumerate(here.others()):
        d_copies[kind].wait_recv()
        halos.append(halo(kind, oa, ob))

    pl.when(above)(up.wait_send)
    pl.when(below)(down.wait_send)
    relay.wait()
    pl.when(below)(from_below.wait)
    pl.when(above)(from_above.wait)
    for copy in d_copies[3:]:
        copy.wait_recv()
    for copy in d_copies:
        copy.wait_send()
    for copy, sends, gets in halos:
        pl.when(sends)(copy.wait_send)
        pl.when(gets)(copy.wait_recv)


def sides(product):
    half = product.shape[1] // 2
    return product[:, :half] + product[:, half:]


def stack(product):
    half = product.shape[0] // 2
    return product[:half] + product[half:]


def iteration_kernel(est_ref, data_ref, lz_ref, x_ref, ly_ref, lyb_ref, xb_ref, lzb_ref,
                     out_ref, t_ref, s_ref):
    wide, deep, lanes = est_ref.shape
    _, outer, tall, _ = data_ref.shape
    rows, planes, _ = out_ref.shape
    t_stride = t_ref.shape[1] // wide
    s_stride = s_ref.shape[1] // outer
    cut = lambda value, count: [value[:, i * lanes:(i + 1) * lanes] for i in range(count)]

    @pl.loop(0, wide // GROUP)
    def _(step):
        base = step * GROUP
        right = jnp.concatenate(
            [jnp.concatenate(split(est_ref[base + i]), axis=0) for i in range(GROUP)], axis=1
        )
        for which in range(2):
            along_z = stack(dot(lz_ref[which], right))
            left = jnp.concatenate(split(jnp.concatenate(cut(along_z, GROUP), axis=0)), axis=1)
            along_x = sides(dot(left, x_ref[which]))
            for i in range(GROUP):
                t_ref[which, pl.ds(pl.multiple_of((base + i) * t_stride, 8), outer)] = along_x[i * outer:(i + 1) * outer]

    @pl.loop(0, outer // PLANES)
    def _(step):
        base = step * PLANES
        for which in range(2):
            right = jnp.concatenate([
                jnp.concatenate(split(t_ref[which, pl.ds(base + i, wide, stride=t_stride)]), axis=0)
                for i in range(PLANES)
            ], axis=1)
            blurred = stack(dot(ly_ref[which], right))
            data = jnp.concatenate([data_ref[which, base + i] for i in range(PLANES)], axis=1)
            right = jnp.concatenate(split(data / blurred), axis=0)
            along_y = stack(dot(lyb_ref[which], right))
            left = jnp.concatenate(split(jnp.concatenate(cut(along_y, PLANES), axis=0)), axis=1)
            along_x = sides(dot(left, xb_ref[which]))
            for i in range(PLANES):
                s_ref[which, pl.ds(pl.multiple_of((base + i) * s_stride, 8), rows)] = along_x[i * rows:(i + 1) * rows]

    @pl.loop(0, rows // GROUP)
    def _(step):
        base = step * GROUP
        both = []
        for which in range(2):
            right = jnp.concatenate([
                jnp.concatenate(split(s_ref[which, pl.ds(base + i, outer, stride=s_stride)]), axis=0)
                for i in range(GROUP)
            ], axis=1)
            both.append(stack(dot(lzb_ref[which], right)))
        for i, piece in enumerate(cut(both[0] * both[1], GROUP)):
            out_ref[base + i] = piece


def root(value):
    return jnp.sqrt(jnp.sqrt(value))


def swap_and_update(here, product_ref, other_ref, sems, update, first):
    rows = product_ref.shape[0]
    chunks = 4
    size = rows // chunks
    copies = []
    for i in range(chunks):
        at = pl.ds(i * size, size)
        copy = remote(product_ref.at[at], other_ref.at[at], sems, first + i, here.partner())
        copy.start()
        copies.append(copy)
    for i in range(chunks):
        copies[i].wait_recv()

        @pl.loop(0, size)
        def _(row):
            update(i * size + row, root(product_ref[i * size + row] * other_ref[i * size + row]))
    return copies


def middle_kernel(blocks, product_ref, old_ref, est_ref, other_ref, p_s, p_r, y_s, y_r, z_s, z_r, q_s, q_r):
    here = Place(blocks)
    rows, depth, lanes = product_ref.shape
    wide, deep, _ = old_ref.shape
    reach = (wide - rows) // 2
    k, c, strip = here.k, here.c, here.strip
    below, above = k > 0, k < blocks - 1
    left, right = strip > 0, strip < 3
    inside = pl.ds(reach, depth)
    greet(here, True, True, False)

    def update(row, factor):
        est_ref[reach + row, inside] = old_ref[reach + row, inside] * factor

    product_copies = swap_and_update(here, product_ref, other_ref, (p_s, p_r), update, 0)

    to_left = remote(
        est_ref.at[pl.ds(reach, reach), inside], est_ref.at[pl.ds(reach + rows, reach), inside],
        (y_s, y_r), 0, here.of_strip(strip - 1),
    )
    to_right = remote(
        est_ref.at[pl.ds(rows, reach), inside], est_ref.at[pl.ds(0, reach), inside],
        (y_s, y_r), 1, here.of_strip(strip + 1),
    )
    pl.when(left)(to_left.start)
    pl.when(right)(to_right.start)

    def pair(at, index):
        up = remote(
            est_ref.at[at, pl.ds(depth, reach)], est_ref.at[at, pl.ds(0, reach)],
            (z_s, z_r), index, here.device(k=k + 1),
        )
        down = remote(
            est_ref.at[at, pl.ds(reach, reach)], est_ref.at[at, pl.ds(reach + depth, reach)],
            (z_s, z_r), index + 1, here.device(k=k - 1),
        )
        from_below = remote(
            est_ref.at[at, pl.ds(0, reach)], est_ref.at[at, pl.ds(0, reach)],
            (q_s, q_r), index, here.partner(),
        )
        from_above = remote(
            est_ref.at[at, pl.ds(reach + depth, reach)], est_ref.at[at, pl.ds(reach + depth, reach)],
            (q_s, q_r), index + 1, here.partner(),
        )
        return up, down, from_below, from_above

    main = pair(pl.ds(reach + c * (rows // 2), rows // 2), 0)
    pl.when(above)(main[0].start)
    pl.when(below)(main[1].start)

    def zero(first_row, count, first, size):
        @pl.loop(0, count)
        def _(row):
            est_ref[first_row + row, pl.ds(first, size)] = jnp.zeros((size, lanes), jnp.float32)

    pl.when(jnp.logical_not(left))(lambda: zero(0, reach, reach, depth))
    pl.when(jnp.logical_not(right))(lambda: zero(reach + rows, reach, reach, depth))
    pl.when(jnp.logical_not(below))(lambda: zero(0, wide, 0, reach))
    pl.when(jnp.logical_not(above))(lambda: zero(0, wide, reach + depth, reach))

    pl.when(left)(to_right.wait_recv)
    pl.when(right)(to_left.wait_recv)
    corner = pair(pl.ds(c * (reach + rows), reach), 2)
    pl.when(above)(corner[0].start)
    pl.when(below)(corner[1].start)

    for up, down, from_below, from_above in (main, corner):
        @pl.when(below)
        def _():
            up.wait_recv()
            from_below.start()

        @pl.when(above)
        def _():
            down.wait_recv()
            from_above.start()

    for copy in product_copies:
        copy.wait_send()
    pl.when(left)(to_left.wait_send)
    pl.when(right)(to_right.wait_send)
    for up, down, from_below, from_above in (main, corner):
        pl.when(above)(up.wait_send)
        pl.when(below)(down.wait_send)
        pl.when(below)(from_below.wait)
        pl.when(above)(from_above.wait)


def last_kernel(blocks, product_ref, old_ref, all_ref, other_ref, new_ref, p_s, p_r, g_s, g_r, q_s, q_r):
    here = Place(blocks)
    rows, depth, lanes = product_ref.shape
    wide = old_ref.shape[0]
    reach = (wide - rows) // 2
    planes = depth // 2
    a, b, c, strip = here.a, here.b, here.c, here.strip
    greet(here, False, False, True)

    def update(row, factor):
        new_ref[row] = old_ref[reach + row, pl.ds(reach, depth)] * factor

    product_copies = swap_and_update(here, product_ref, other_ref, (p_s, p_r), update, 0)
    half = rows // 2
    copies = []
    for kind, (oa, ob) in enumerate(here.others()):
        copy = remote(
            new_ref.at[pl.ds(half * c, half), pl.ds(pl.multiple_of(planes * ob, 8), planes)],
            all_ref.at[pl.ds(rows * strip + half * c, half), pl.ds(0, planes)],
            (g_s, g_r), kind, here.device(a=oa, b=ob),
        )
        copy.start()
        copies.append(copy)

    @pl.loop(0, rows)
    def _(row):
        all_ref[rows * strip + row, pl.ds(0, planes)] = new_ref[row, pl.ds(pl.multiple_of(planes * b, 8), planes)]

    relays = []
    for kind, (oa, ob) in enumerate(here.others()):
        copies[kind].wait_recv()
        at = pl.ds(rows * here.strip_of(oa, ob) + half * c, half)
        relay = remote(
            all_ref.at[at, pl.ds(0, planes)], all_ref.at[at, pl.ds(0, planes)],
            (q_s, q_r), kind, here.partner(),
        )
        relay.start()
        relays.append(relay)
    for copy in product_copies + copies:
        copy.wait_send()
    for relay in relays:
        relay.wait()


def output_kernel(all_ref, out_ref):
    group, lanes, width = out_ref.shape
    stride = all_ref.shape[0] // width
    base = pl.program_id(0) * group
    for i in range(group):
        out_ref[i] = all_ref[pl.ds(base + i, width, stride=stride)].T


def on_device(sections, count, views_data, start, psf_table, psf_index):
    f32, bf16 = jnp.float32, jnp.bfloat16
    planes, width_x, width_y = start.shape
    taps = psf_table.shape[2]
    reach = taps - 1
    pad = reach // 2
    blocks = count // 2
    rows = width_y // 4
    depth = 2 * planes
    wide, deep = rows + 2 * reach, depth + 2 * reach
    tall, outer = rows + 2 * pad, depth + 2 * pad
    shape = jax.ShapeDtypeStruct
    dma = lambda n: [pltpu.SemaphoreType.DMA((n,)), pltpu.SemaphoreType.DMA((n,))]
    stride = odd_stride(planes)

    kern = jnp.sum(jnp.where(jnp.arange(psf_table.shape[0])[:, None, None] == psf_index[0], psf_table, 0.0), axis=0)
    kern = kern / jnp.sum(kern, axis=-1, keepdims=True)
    kern = jnp.pad(kern, ((0, 8 - kern.shape[0]), (0, 128 - taps)))

    est, data, *matrices = pl.pallas_call(
        functools.partial(setup_kernel, blocks, taps, rows),
        out_shape=[
            shape((wide, deep, width_x), f32),
            shape((2, outer, tall, width_x), f32),
            shape((2, 2 * outer, 2 * deep), bf16),
            shape((2, 2 * width_x, 2 * width_x), bf16),
            shape((2, 2 * tall, 2 * wide), bf16),
            shape((2, 2 * rows, 2 * tall), bf16),
            shape((2, 2 * width_x, 2 * width_x), bf16),
            shape((2, 2 * depth, 2 * outer), bf16),
        ],
        in_specs=[ANY, ANY, VMEM],
        out_specs=[VMEM] * 8,
        scratch_shapes=[
            pltpu.VMEM(start.shape, f32),
            pltpu.VMEM(start.shape, f32),
            pltpu.VMEM(((width_y + 2 * reach) * stride, width_x), f32),
            pltpu.VMEM((planes, width_y + 2 * pad, width_x), f32),
            pltpu.VMEM((2, 8, 128), f32),
            pltpu.SemaphoreType.DMA((2,)),
            *dma(1), *dma(6), *dma(6), *dma(4),
        ],
        compiler_params=pltpu.CompilerParams(
            collective_id=0, has_side_effects=True, vmem_limit_bytes=40 * MIB
        ),
    )(views_data[0], start, kern)

    for step in range(ITERS):
        product = pl.pallas_call(
            iteration_kernel,
            out_shape=shape((rows, depth, width_x), f32),
            in_specs=[VMEM] * 8,
            out_specs=VMEM,
            scratch_shapes=[
                pltpu.VMEM((2, wide * odd_stride(outer), width_x), f32),
                pltpu.VMEM((2, outer * odd_stride(rows), width_x), f32),
            ],
            compiler_params=pltpu.CompilerParams(vmem_limit_bytes=40 * MIB),
        )(est, data, *matrices)
        if step < ITERS - 1:
            est = pl.pallas_call(
                functools.partial(middle_kernel, blocks),
                out_shape=shape(est.shape, f32),
                in_specs=[VMEM] * 2,
                out_specs=VMEM,
                scratch_shapes=[
                    pltpu.VMEM(product.shape, f32), *dma(4), *dma(2), *dma(4), *dma(4),
                ],
                compiler_params=pltpu.CompilerParams(
                    collective_id=1, has_side_effects=True, vmem_limit_bytes=40 * MIB
                ),
            )(product, est)

    gathered = pl.pallas_call(
        functools.partial(last_kernel, blocks),
        out_shape=shape((width_y, stride, width_x), f32),
        in_specs=[VMEM] * 2,
        out_specs=VMEM,
        scratch_shapes=[
            pltpu.VMEM(product.shape, f32), pltpu.VMEM(product.shape, f32), *dma(4), *dma(3), *dma(3),
        ],
        compiler_params=pltpu.CompilerParams(
            collective_id=2, has_side_effects=True, vmem_limit_bytes=40 * MIB
        ),
    )(product, est)
    return pl.pallas_call(
        output_kernel,
        grid=(planes // 4,),
        out_shape=shape(start.shape, f32),
        in_specs=[VMEM],
        out_specs=pl.BlockSpec((4, width_x, width_y), lambda i: (i, 0, 0)),
        compiler_params=pltpu.CompilerParams(vmem_limit_bytes=40 * MIB),
    )(gathered.reshape(width_y * stride, width_x))


def solution(mesh):
    return jax.shard_map(
        functools.partial(on_device, mesh.shape["view"], mesh.shape["gz"]),
        mesh=mesh,
        in_specs=(P("view", "gz", None, None), P("gz", None, None), P(), P("view")),
        out_specs=P("gz", None, None),
        check_vma=False,
    )
```

```python
import functools
import jax
import jax.numpy as jnp
from jax import lax
from jax.experimental import pallas as pl
from jax.experimental.pallas import tpu as pltpu
from jax.sharding import PartitionSpec as P

ITERS = 2
GROUP = 32
MESH = pl.DeviceIdType.MESH
VMEM = pl.BlockSpec(memory_space=pltpu.VMEM)
HBM = pl.BlockSpec(memory_space=pltpu.HBM)
VMEM_LIMIT = 56
MIB = 1024 * 1024


def split(value):
    high = value.astype(jnp.bfloat16)
    return high, (value - high.astype(jnp.float32)).astype(jnp.bfloat16)


def dot(lhs, rhs):
    return jnp.dot(lhs, rhs, preferred_element_type=jnp.float32)


def odd_stride(rows):
    return rows + 8 if (rows // 8) % 2 == 0 else rows


class Place:
    def __init__(self, blocks):
        view, gz = lax.axis_index("view"), lax.axis_index("gz")
        self.blocks = blocks
        self.a, self.c = view // 2, view % 2
        self.k, self.b = gz // 2, gz % 2
        self.strip = self.strip_of(self.a, self.b)

    @staticmethod
    def strip_of(a, b):
        return 2 * a + (a + b) % 2

    def device(self, a=None, c=None, k=None, b=None):
        a = self.a if a is None else a
        c = self.c if c is None else c
        k = self.k if k is None else k
        b = self.b if b is None else b
        return (2 * a + c, 2 * k + b)

    def of_strip(self, strip):
        return self.device(a=strip // 2, b=(strip % 2 + strip // 2) % 2)

    def partner(self):
        return self.device(c=1 - self.c)

    def others(self):
        a, b = self.a, self.b
        return ((a, 1 - b), (1 - a, b), (1 - a, 1 - b))


def remote(src, dst, sems, index, device):
    send, recv = sems
    return pltpu.make_async_remote_copy(
        src_ref=src, dst_ref=dst, send_sem=send.at[index], recv_sem=recv.at[index],
        device_id=device, device_id_type=MESH,
    )


def greet(here):
    barrier = pltpu.get_barrier_semaphore()

    def signal(device):
        pl.semaphore_signal(barrier, inc=1, device_id=device, device_id_type=MESH)

    signal(here.partner())
    count = 1
    for a, b in here.others():
        signal(here.device(a=a, b=b))
        count += 1
    for step in (-1, 1):
        there = here.k + step
        inside = (there >= 0) & (there < here.blocks)
        pl.when(inside)(functools.partial(lambda there: signal(here.device(k=there)), there))
        count = count + inside.astype(jnp.int32)
    pl.semaphore_wait(barrier, count)


def band(taps, outputs, inputs, sign, shift):
    at = sign * (
        lax.broadcasted_iota(jnp.int32, (outputs, inputs), 1)
        - lax.broadcasted_iota(jnp.int32, (outputs, inputs), 0)
    ) + shift
    total = jnp.zeros((outputs, inputs), jnp.float32)
    for tap, value in enumerate(taps):
        total = jnp.where(at == tap, value, total)
    return total


def write_left(ref, index, matrix):
    high, low = split(matrix)
    rows, depth = matrix.shape
    top = jnp.concatenate([high, high], axis=1)
    bottom = jnp.concatenate([low, low], axis=1)
    ref[index] = jnp.concatenate([top, bottom], axis=0)


def write_right(ref, index, matrix):
    high, low = split(matrix)
    half = jnp.concatenate([high, low], axis=1)
    ref[index] = jnp.concatenate([half, half], axis=0)


def write_matrices(kern_ref, taps, refs):
    lz_ref, x_ref, ly_ref, lyb_ref, xb_ref, lzb_ref = refs
    reach = taps - 1
    pad = reach // 2
    for which in range(2):
        rows = kern_ref[which]
        kz, kx, ky = ([rows[r:r + 1, t:t + 1] for t in range(taps)] for r in range(3))
        outputs, inputs = lz_ref.shape[1] // 2, lz_ref.shape[2] // 2
        write_left(lz_ref, which, band(kz, outputs, inputs, 1, 0))
        write_right(x_ref, which, band(kx, x_ref.shape[1] // 2, x_ref.shape[2] // 2, -1, pad))
        write_left(ly_ref, which, band(ky, ly_ref.shape[1] // 2, ly_ref.shape[2] // 2, 1, 0))
        write_left(lyb_ref, which, band(ky, lyb_ref.shape[1] // 2, lyb_ref.shape[2] // 2, -1, reach))
        write_right(xb_ref, which, band(kx, xb_ref.shape[1] // 2, xb_ref.shape[2] // 2, 1, pad))
        write_left(lzb_ref, which, band(kz, lzb_ref.shape[1] // 2, lzb_ref.shape[2] // 2, -1, reach))


def sides(product):
    half = product.shape[1] // 2
    return product[:, :half] + product[:, half:]


def stack(product):
    half = product.shape[0] // 2
    return product[:half] + product[half:]


def cut(value, count):
    lanes = value.shape[1] // count
    return [value[:, i * lanes:(i + 1) * lanes] for i in range(count)]


def stacked(values):
    return jnp.concatenate([jnp.concatenate(split(value), axis=0) for value in values], axis=1)


def beside(pieces):
    return jnp.concatenate(split(jnp.concatenate(pieces, axis=0)), axis=1)


def root(value):
    return jnp.sqrt(jnp.sqrt(value))


def forward_rows(base, count, est_ref, lz_ref, x_ref, t_ref):
    outer = lz_ref.shape[1] // 2
    stride = t_ref.shape[1] // est_ref.shape[0]
    left = lz_ref[...].reshape(4 * outer, lz_ref.shape[2])
    both = dot(left, stacked([est_ref[base + i] for i in range(count)]))
    for which in range(2):
        along_z = stack(both[2 * outer * which:2 * outer * (which + 1)])
        along_x = sides(dot(beside(cut(along_z, count)), x_ref[which]))
        for i in range(count):
            t_ref[which, pl.ds(pl.multiple_of((base + i) * stride, 8), outer)] = along_x[i * outer:(i + 1) * outer]


def ratio_planes(planes, data_ref, ly_ref, lyb_ref, xb_ref, t_ref, s_ref):
    count = len(planes)
    wide, rows = ly_ref.shape[2] // 2, lyb_ref.shape[1] // 2
    t_stride = t_ref.shape[1] // wide
    s_stride = s_ref.shape[1] // data_ref.shape[1]
    for which in range(2):
        right = stacked([t_ref[which, pl.ds(plane, wide, stride=t_stride)] for plane in planes])
        blurred = stack(dot(ly_ref[which], right))
        data = jnp.concatenate([data_ref[which, plane] for plane in planes], axis=1)
        right = jnp.concatenate(split(data / blurred), axis=0)
        along_y = stack(dot(lyb_ref[which], right))
        along_x = sides(dot(beside(cut(along_y, count)), xb_ref[which]))
        for i, plane in enumerate(planes):
            s_ref[which, pl.ds(pl.multiple_of(plane * s_stride, 8), rows)] = along_x[i * rows:(i + 1) * rows]


def back_rows(base, count, lzb_ref, s_ref, product_ref):
    outer = lzb_ref.shape[2] // 2
    stride = s_ref.shape[1] // outer
    both = []
    for which in range(2):
        right = stacked([s_ref[which, pl.ds(base + i, outer, stride=stride)] for i in range(count)])
        both.append(stack(dot(lzb_ref[which], right)))
    for i, piece in enumerate(cut(both[0] * both[1], count)):
        product_ref[base + i] = piece


def whole_kernel(blocks, strip_rows, data_hbm, start_hbm, table_ref, index_ref,
                 all_ref,
                 sbuf, dbuf, ts_ref, td_ref, kern_ref, est_ref, est2_ref, data_ref,
                 lz_ref, x_ref, ly_ref, lyb_ref, xb_ref, lzb_ref, t_ref, s_ref,
                 product_ref, other_ref, other2_ref,
                 load_sem, kern_s, kern_r, e_s, e_r, d_s, d_r, h_s, h_r,
                 p_s, p_r, y_s, y_r, z_s, z_r, q_s, q_r, f_s, f_r, g_s, g_r, o_s, o_r, w_s, w_r):
    here = Place(blocks)
    planes, width_x, width_y = start_hbm.shape
    taps = table_ref.shape[2]
    reach = taps - 1
    pad = reach // 2
    depth = 2 * planes
    rows = strip_rows
    wide = rows + 2 * reach
    tall = rows + 2 * pad
    stride = ts_ref.shape[0] // (width_y + 2 * reach)
    half = wide // 2
    k, a, b, c, strip = here.k, here.a, here.b, here.c, here.strip
    below, above = k > 0, k < blocks - 1
    unless = lambda condition: pl.when(jnp.logical_not(condition))
    load_start = pltpu.make_async_copy(start_hbm, sbuf, load_sem.at[0])
    load_data = pltpu.make_async_copy(data_hbm, dbuf, load_sem.at[1])
    load_start.start()
    load_data.start()
    ts3 = ts_ref.reshape(width_y + 2 * reach, stride, width_x)

    table = table_ref[...]
    kern = jnp.zeros(table.shape[1:], jnp.float32)
    for i in range(table.shape[0]):
        kern = jnp.where(index_ref[0] == i, table[i], kern)
    kern = kern / jnp.sum(kern, axis=-1, keepdims=True)
    kern_ref[a] = jnp.zeros(kern_ref.shape[1:], jnp.float32)
    kern_ref[a, pl.ds(0, 3), pl.ds(0, taps)] = kern
    ts_ref[pl.ds(0, reach * stride)] = jnp.zeros((reach * stride, width_x), jnp.float32)
    ts_ref[pl.ds((width_y + reach) * stride, reach * stride)] = jnp.zeros((reach * stride, width_x), jnp.float32)
    for z in range(planes):
        td_ref[z, pl.ds(0, pad)] = jnp.zeros((pad, width_x), jnp.float32)
        td_ref[z, pl.ds(pad + width_y, pad)] = jnp.zeros((pad, width_x), jnp.float32)
    greet(here)

    load_start.wait()

    @pl.loop(0, planes)
    def _(z):
        ts_ref[pl.ds(reach * stride + z, width_y, stride=stride)] = sbuf[z].T

    mine = pl.multiple_of(reach + planes * b, 8)
    theirs = pl.multiple_of(reach + planes * (1 - b), 8)
    rows_c = pl.ds(half * c, half)
    e_copy = remote(
        ts3.at[pl.ds(rows * here.strip_of(a, 1 - b) + half * c, half), pl.ds(0, planes)],
        est_ref.at[rows_c, pl.ds(mine, planes)], (e_s, e_r), 0, here.device(b=1 - b),
    )
    e_copy.start()
    kern_copy = remote(kern_ref.at[a], kern_ref.at[a], (kern_s, kern_r), 0, here.device(a=1 - a))
    kern_copy.start()

    load_data.wait()

    @pl.loop(0, planes)
    def _(z):
        td_ref[z, pl.ds(pad, width_y)] = dbuf[z].T

    d_copies = []
    for part, (first, size) in enumerate(((b * (planes - pad), pad), ((1 - b) * pad, planes - pad))):
        for kind, (oa, ob) in enumerate(here.others()):
            copy = remote(
                td_ref.at[pl.ds(first, size), pl.ds(rows * here.strip_of(oa, ob), tall)],
                data_ref.at[a, pl.ds(pad + planes * b + first, size)],
                (d_s, d_r), 3 * part + kind, here.device(a=oa, b=ob),
            )
            copy.start()
            d_copies.append(copy)

    @pl.loop(0, wide)
    def _(row):
        est_ref[row, pl.ds(mine, planes)] = ts3[rows * strip + row, pl.ds(0, planes)]

    @pl.loop(0, planes)
    def _(z):
        data_ref[a, pad + planes * b + z] = td_ref[z, pl.ds(pl.multiple_of(rows * strip, 8), tall)]

    def zero(ref, first_row, count, first, size):
        @pl.loop(0, count)
        def _(row):
            ref[first_row + row, pl.ds(first, size)] = jnp.zeros((size, width_x), jnp.float32)

    unless(below)(lambda: zero(est_ref, 0, wide, 0, reach))
    unless(above)(lambda: zero(est_ref, 0, wide, reach + depth, reach))

    def halo(kind, oa, ob):
        to = k + 2 * ob - 1
        source = k + 1 - 2 * ob
        place = (1 - ob) * (depth + pad)
        copy = remote(
            data_ref.at[oa, pl.ds(pad + ob * (depth - pad), pad)], data_ref.at[oa, pl.ds(place, pad)],
            (h_s, h_r), kind, here.device(k=to),
        )
        sends = (to >= 0) & (to < blocks)
        gets = (source >= 0) & (source < blocks)
        unless(gets)(lambda: zero(data_ref.at[oa], place, pad, 0, tall))
        pl.when(sends)(copy.start)
        return copy, sends, gets

    halos = [halo(3, a, b)]

    kern_copy.wait()
    write_matrices(kern_ref, taps, (lz_ref, x_ref, ly_ref, lyb_ref, xb_ref, lzb_ref))

    e_copy.wait()
    relay = remote(
        est_ref.at[rows_c, pl.ds(theirs, planes)], est_ref.at[rows_c, pl.ds(theirs, planes)],
        (e_s, e_r), 1, here.partner(),
    )
    bottom, top = pl.ds(0, reach), pl.ds(reach + depth, reach)
    first, last = pl.ds(reach, reach), pl.ds(depth, reach)
    up = remote(est_ref.at[rows_c, last], est_ref.at[rows_c, bottom], (e_s, e_r), 2, here.device(k=k + 1))
    down = remote(est_ref.at[rows_c, first], est_ref.at[rows_c, top], (e_s, e_r), 3, here.device(k=k - 1))
    from_below = remote(est_ref.at[rows_c, bottom], est_ref.at[rows_c, bottom], (e_s, e_r), 4, here.partner())
    from_above = remote(est_ref.at[rows_c, top], est_ref.at[rows_c, top], (e_s, e_r), 5, here.partner())
    pl.when(above)(up.start)
    pl.when(below)(down.start)
    relay.start()

    @pl.when(below)
    def _():
        up.wait_recv()
        from_below.start()

    @pl.when(above)
    def _():
        down.wait_recv()
        from_above.start()

    pl.when(above)(up.wait_send)
    pl.when(below)(down.wait_send)
    relay.wait()
    pl.when(below)(from_below.wait)
    pl.when(above)(from_above.wait)

    @pl.loop(0, wide // GROUP)
    def _(step):
        forward_rows(step * GROUP, GROUP, est_ref, lz_ref, x_ref, t_ref)

    def back_planes(base, other):
        ratio_planes(
            [base + i for i in range(pad)] + [other + i for i in range(pad)],
            data_ref, ly_ref, lyb_ref, xb_ref, t_ref, s_ref,
        )

    steps = planes // pad + 1
    for kind, (oa, ob) in enumerate(here.others()):
        d_copies[kind].wait_recv()
        halos.append(halo(kind, oa, ob))

    @pl.loop(0, steps)
    def _(step):
        @pl.when(step == 1)
        def _():
            for copy in d_copies[3:]:
                copy.wait_recv()

        @pl.when(step == steps - 1)
        def _():
            for copy, sends, gets in halos:
                pl.when(gets)(copy.wait_recv)

        outside, edge = step == steps - 1, step == 0
        back_planes(
            jnp.where(outside, 0, jnp.where(edge, pad, 2 * pad * step)),
            jnp.where(outside, depth + pad, jnp.where(edge, depth, 2 * pad * step + pad)),
        )

    chunks = rows // reach
    inside = pl.ds(reach, depth)
    left, right = strip > 0, strip < 3

    def chunk_of(i):
        middle = jnp.where(i == 0, 1, jnp.where(i == 1, chunks, i))
        return jnp.where(i == chunks, 0, jnp.where(i == chunks + 1, chunks + 1, middle))

    def swap(q):
        at = pl.ds(reach * q, reach)
        return remote(product_ref.at[at], other_ref.at[at], (p_s, p_r), q, here.partner())

    @pl.loop(0, chunks)
    def _(i):
        q = chunk_of(i) - 1
        back_rows(reach * q, reach, lzb_ref, s_ref, product_ref)
        swap(q).start()

    unless(left)(lambda: zero(est2_ref, 0, reach, reach, depth))
    unless(right)(lambda: zero(est2_ref, reach + rows, reach, reach, depth))
    unless(below)(lambda: zero(est2_ref, 0, wide, 0, reach))
    unless(above)(lambda: zero(est2_ref, 0, wide, reach + depth, reach))

    to_left = remote(
        est2_ref.at[pl.ds(reach, reach), inside], est2_ref.at[pl.ds(reach + rows, reach), inside],
        (y_s, y_r), 0, here.of_strip(strip - 1),
    )
    to_right = remote(
        est2_ref.at[pl.ds(rows, reach), inside], est2_ref.at[pl.ds(0, reach), inside],
        (y_s, y_r), 1, here.of_strip(strip + 1),
    )
    to_block = k + 1 - 2 * c
    z_sends = (to_block >= 0) & (to_block < blocks)
    z_gets = (k - 1 + 2 * c >= 0) & (k - 1 + 2 * c < blocks)
    q_gets = (k + 1 - 2 * c >= 0) & (k + 1 - 2 * c < blocks)
    z_from = pl.multiple_of(reach + (1 - c) * (depth - reach), 8)
    z_to = pl.multiple_of(c * (reach + depth), 8)

    def along_z(e):
        at = pl.ds(reach * e, reach)
        return remote(
            est2_ref.at[at, pl.ds(z_from, reach)], est2_ref.at[at, pl.ds(z_to, reach)],
            (z_s, z_r), e, here.device(k=to_block),
        )

    def across(e):
        at = pl.ds(reach * e, reach)
        return remote(
            est2_ref.at[at, pl.ds(z_to, reach)], est2_ref.at[at, pl.ds(z_to, reach)],
            (q_s, q_r), e, here.partner(),
        )

    @pl.loop(0, chunks)
    def _(i):
        e = chunk_of(i)
        q = e - 1
        swap(q).wait_recv()

        @pl.loop(0, reach)
        def _(r):
            row = reach * q + r
            factor = root(product_ref[row] * other_ref[row])
            est2_ref[reach + row, inside] = est_ref[reach + row, inside] * factor

        pl.when((i == 0) & left)(to_left.start)
        pl.when((i == 1) & right)(to_right.start)
        pl.when(z_sends)(along_z(e).start)

    pl.when(left)(to_right.wait_recv)
    pl.when(right)(to_left.wait_recv)
    pl.when(z_sends)(along_z(0).start)
    pl.when(z_sends)(along_z(chunks + 1).start)

    @pl.loop(0, chunks + 3)
    def _(i):
        @pl.when((i < chunks + 2) & z_gets)
        def _():
            e = chunk_of(i)
            along_z(e).wait_recv()
            across(e).start()

        @pl.when(i >= 1)
        def _():
            e = chunk_of(i - 1)
            pl.when(q_gets)(across(e).wait_recv)
            forward_rows(reach * e, reach, est2_ref, lz_ref, x_ref, t_ref)

    @pl.loop(0, chunks)
    def _(q):
        swap(q).wait_send()

    @pl.loop(0, steps)
    def _(step):
        back_planes(2 * pad * step, 2 * pad * step + pad)

    part = reach // 2

    def last_swap(q):
        at = pl.ds(reach * q + part * (1 - c), part)
        return remote(product_ref.at[at], other2_ref.at[at], (f_s, f_r), q, here.partner())

    def gather(q, kind, oa, ob):
        return remote(
            other2_ref.at[pl.ds(reach * q + part * c, part), pl.ds(pl.multiple_of(planes * ob, 8), planes)],
            all_ref.at[pl.ds(rows * strip + reach * q + part * c, part)],
            (g_s, g_r), 3 * q + kind, here.device(a=oa, b=ob),
        )

    def own(q):
        return remote(
            other2_ref.at[pl.ds(reach * q + part * c, part), pl.ds(pl.multiple_of(planes * b, 8), planes)],
            all_ref.at[pl.ds(rows * strip + reach * q + part * c, part)],
            (o_s, o_r), q, here.partner(),
        )

    def onward(q, kind, oa, ob):
        at = pl.ds(rows * here.strip_of(oa, ob) + reach * q + part * c, part)
        return remote(all_ref.at[at], all_ref.at[at], (w_s, w_r), 3 * q + kind, here.partner())

    @pl.loop(0, chunks)
    def _(q):
        back_rows(reach * q, reach, lzb_ref, s_ref, product_ref)
        last_swap(q).start()

    @pl.loop(0, chunks)
    def _(q):
        last_swap(q).wait_recv()

        @pl.loop(0, part)
        def _(r):
            row = reach * q + part * c + r
            factor = root(product_ref[row] * other2_ref[row])
            other2_ref[row] = est2_ref[reach + row, inside] * factor
            all_ref[rows * strip + row] = other2_ref[row, pl.ds(pl.multiple_of(planes * b, 8), planes)]

        for kind in (2, 0, 1):
            gather(q, kind, *here.others()[kind]).start()
        own(q).start()

    @pl.loop(0, chunks)
    def _(q):
        for kind in range(3):
            gather(q, kind, *here.others()[kind]).wait_recv()
            onward(q, kind, *here.others()[kind]).start()

    @pl.loop(0, chunks)
    def _(q):
        last_swap(q).wait_send()
        own(q).wait()
        for kind in range(3):
            gather(q, kind, *here.others()[kind]).wait_send()
            onward(q, kind, *here.others()[kind]).wait()

    for copy in d_copies:
        copy.wait_send()
    for copy, sends, gets in halos:
        pl.when(sends)(copy.wait_send)
    pl.when(left)(to_left.wait_send)
    pl.when(right)(to_right.wait_send)

    @pl.loop(0, chunks + 2)
    def _(e):
        pl.when(z_sends)(along_z(e).wait_send)
        pl.when(z_gets)(across(e).wait_send)


def output_kernel(all_ref, out_ref):
    group, lanes, width = out_ref.shape
    stride = all_ref.shape[0] // width
    base = pl.program_id(0) * group
    for i in range(group):
        out_ref[i] = all_ref[pl.ds(base + i, width, stride=stride)].T


def on_device(blocks, views_data, start, psf_table, psf_index):
    f32, bf16 = jnp.float32, jnp.bfloat16
    planes, width_x, width_y = start.shape
    reach = psf_table.shape[2] - 1
    pad = reach // 2
    rows = width_y // 4
    depth = 2 * planes
    wide, deep = rows + 2 * reach, depth + 2 * reach
    tall, outer = rows + 2 * pad, depth + 2 * pad
    chunks = rows // reach
    dma = lambda n: [pltpu.SemaphoreType.DMA((n,)), pltpu.SemaphoreType.DMA((n,))]

    gathered = pl.pallas_call(
        functools.partial(whole_kernel, blocks, rows),
        out_shape=jax.ShapeDtypeStruct((width_y, planes, width_x), f32),
        in_specs=[HBM, HBM, VMEM, pl.BlockSpec(memory_space=pltpu.SMEM)],
        out_specs=VMEM,
        scratch_shapes=[
            pltpu.VMEM(start.shape, f32),
            pltpu.VMEM(start.shape, f32),
            pltpu.VMEM(((width_y + 2 * reach) * odd_stride(planes), width_x), f32),
            pltpu.VMEM((planes, width_y + 2 * pad, width_x), f32),
            pltpu.VMEM((2, 8, 128), f32),
            pltpu.VMEM((wide, deep, width_x), f32),
            pltpu.VMEM((wide, deep, width_x), f32),
            pltpu.VMEM((2, outer, tall, width_x), f32),
            pltpu.VMEM((2, 2 * outer, 2 * deep), bf16),
            pltpu.VMEM((2, 2 * width_x, 2 * width_x), bf16),
            pltpu.VMEM((2, 2 * tall, 2 * wide), bf16),
            pltpu.VMEM((2, 2 * rows, 2 * tall), bf16),
            pltpu.VMEM((2, 2 * width_x, 2 * width_x), bf16),
            pltpu.VMEM((2, 2 * depth, 2 * outer), bf16),
            pltpu.VMEM((2, wide * odd_stride(outer), width_x), f32),
            pltpu.VMEM((2, outer * odd_stride(rows), width_x), f32),
            pltpu.VMEM((rows, depth, width_x), f32),
            pltpu.VMEM((rows, depth, width_x), f32),
            pltpu.VMEM((rows, depth, width_x), f32),
            pltpu.SemaphoreType.DMA((2,)),
            *dma(1), *dma(6), *dma(6), *dma(4),
            *dma(chunks), *dma(2), *dma(chunks + 2), *dma(chunks + 2),
            *dma(chunks), *dma(3 * chunks), *dma(chunks), *dma(3 * chunks),
        ],
        compiler_params=pltpu.CompilerParams(
            collective_id=0, has_side_effects=True, vmem_limit_bytes=VMEM_LIMIT * MIB
        ),
    )(views_data[0], start, psf_table, psf_index)
    return pl.pallas_call(
        output_kernel,
        grid=(planes // 4,),
        out_shape=jax.ShapeDtypeStruct(start.shape, f32),
        in_specs=[VMEM],
        out_specs=pl.BlockSpec((4, width_x, width_y), lambda i: (i, 0, 0)),
        compiler_params=pltpu.CompilerParams(vmem_limit_bytes=12 * MIB),
    )(gathered.reshape(width_y * planes, width_x))


def solution(mesh):
    return jax.shard_map(
        functools.partial(on_device, mesh.shape["gz"] // 2),
        mesh=mesh,
        in_specs=(P("view", "gz", None, None), P("gz", None, None), P(), P("view")),
        out_specs=P("gz", None, None),
        check_vma=False,
    )
```

```python
import functools
import jax
import jax.numpy as jnp
from jax import lax
from jax.experimental import pallas as pl
from jax.experimental.pallas import tpu as pltpu
from jax.sharding import PartitionSpec as P

ITERS = 2
GROUP = 32
MESH = pl.DeviceIdType.MESH
VMEM = pl.BlockSpec(memory_space=pltpu.VMEM)
HBM = pl.BlockSpec(memory_space=pltpu.HBM)
VMEM_LIMIT = 48
MIB = 1024 * 1024


def split(value):
    high = value.astype(jnp.bfloat16)
    return high, (value - high.astype(jnp.float32)).astype(jnp.bfloat16)


def dot(lhs, rhs):
    return jnp.dot(lhs, rhs, preferred_element_type=jnp.float32)


def odd_stride(rows):
    return rows + 8 if (rows // 8) % 2 == 0 else rows


class Place:
    def __init__(self, blocks):
        view, gz = lax.axis_index("view"), lax.axis_index("gz")
        self.blocks = blocks
        self.a, self.c = view // 2, view % 2
        self.k, self.b = gz // 2, gz % 2
        self.strip = self.strip_of(self.a, self.b)

    @staticmethod
    def strip_of(a, b):
        return 2 * a + (a + b) % 2

    def device(self, a=None, c=None, k=None, b=None):
        a = self.a if a is None else a
        c = self.c if c is None else c
        k = self.k if k is None else k
        b = self.b if b is None else b
        return (2 * a + c, 2 * k + b)

    def of_strip(self, strip):
        return self.device(a=strip // 2, b=(strip % 2 + strip // 2) % 2)

    def partner(self):
        return self.device(c=1 - self.c)

    def others(self):
        a, b = self.a, self.b
        return ((a, 1 - b), (1 - a, b), (1 - a, 1 - b))


def remote(src, dst, sems, index, device):
    send, recv = sems
    return pltpu.make_async_remote_copy(
        src_ref=src, dst_ref=dst, send_sem=send.at[index], recv_sem=recv.at[index],
        device_id=device, device_id_type=MESH,
    )


def greet(here):
    barrier = pltpu.get_barrier_semaphore()

    def signal(device):
        pl.semaphore_signal(barrier, inc=1, device_id=device, device_id_type=MESH)

    signal(here.partner())
    count = 1
    for a, b in here.others():
        signal(here.device(a=a, b=b))
        count += 1
    for step in (-1, 1):
        there = here.k + step
        inside = (there >= 0) & (there < here.blocks)
        pl.when(inside)(functools.partial(lambda there: signal(here.device(k=there)), there))
        count = count + inside.astype(jnp.int32)
    pl.semaphore_wait(barrier, count)


def band(taps, outputs, inputs, sign, shift):
    at = sign * (
        lax.broadcasted_iota(jnp.int32, (outputs, inputs), 1)
        - lax.broadcasted_iota(jnp.int32, (outputs, inputs), 0)
    ) + shift
    total = jnp.zeros((outputs, inputs), jnp.float32)
    for tap, value in enumerate(taps):
        total = jnp.where(at == tap, value, total)
    return total


def write_left(ref, index, matrix):
    high, low = split(matrix)
    rows, depth = matrix.shape
    top = jnp.concatenate([high, high], axis=1)
    bottom = jnp.concatenate([low, low], axis=1)
    ref[index] = jnp.concatenate([top, bottom], axis=0)


def write_right(ref, index, matrix):
    high, low = split(matrix)
    half = jnp.concatenate([high, low], axis=1)
    ref[index] = jnp.concatenate([half, half], axis=0)


def write_matrices(kern_ref, taps, refs):
    lz_ref, x_ref, ly_ref, lyb_ref, xb_ref, lzb_ref = refs
    reach = taps - 1
    pad = reach // 2
    for which in range(2):
        rows = kern_ref[which]
        kz, kx, ky = ([rows[r:r + 1, t:t + 1] for t in range(taps)] for r in range(3))
        outputs, inputs = lz_ref.shape[1] // 2, lz_ref.shape[2] // 2
        write_left(lz_ref, which, band(kz, outputs, inputs, 1, 0))
        write_right(x_ref, which, band(kx, x_ref.shape[1] // 2, x_ref.shape[2] // 2, -1, pad))
        write_left(ly_ref, which, band(ky, ly_ref.shape[1] // 2, ly_ref.shape[2] // 2, 1, 0))
        write_left(lyb_ref, which, band(ky, lyb_ref.shape[1] // 2, lyb_ref.shape[2] // 2, -1, reach))
        write_right(xb_ref, which, band(kx, xb_ref.shape[1] // 2, xb_ref.shape[2] // 2, 1, pad))
        write_left(lzb_ref, which, band(kz, lzb_ref.shape[1] // 2, lzb_ref.shape[2] // 2, -1, reach))


def sides(product):
    half = product.shape[1] // 2
    return product[:, :half] + product[:, half:]


def stack(product):
    half = product.shape[0] // 2
    return product[:half] + product[half:]


def cut(value, count):
    lanes = value.shape[1] // count
    return [value[:, i * lanes:(i + 1) * lanes] for i in range(count)]


def stacked(values):
    return jnp.concatenate([jnp.concatenate(split(value), axis=0) for value in values], axis=1)


def beside(pieces):
    return jnp.concatenate(split(jnp.concatenate(pieces, axis=0)), axis=1)


def root(value):
    return jnp.sqrt(jnp.sqrt(value))


def forward_rows(base, count, est_ref, lz_ref, x_ref, t_ref):
    outer = lz_ref.shape[1] // 2
    stride = t_ref.shape[1] // est_ref.shape[0]
    left = lz_ref[...].reshape(4 * outer, lz_ref.shape[2])
    both = dot(left, stacked([est_ref[base + i] for i in range(count)]))
    for which in range(2):
        along_z = stack(both[2 * outer * which:2 * outer * (which + 1)])
        along_x = sides(dot(beside(cut(along_z, count)), x_ref[which]))
        for i in range(count):
            t_ref[which, pl.ds(pl.multiple_of((base + i) * stride, 8), outer)] = along_x[i * outer:(i + 1) * outer]


def ratio_planes(planes, data_ref, ly_ref, lyb_ref, xb_ref, t_ref, s_ref):
    count = len(planes)
    wide, rows = ly_ref.shape[2] // 2, lyb_ref.shape[1] // 2
    t_stride = t_ref.shape[1] // wide
    s_stride = s_ref.shape[1] // data_ref.shape[1]
    for which in range(2):
        right = stacked([t_ref[which, pl.ds(plane, wide, stride=t_stride)] for plane in planes])
        blurred = stack(dot(ly_ref[which], right))
        data = jnp.concatenate([data_ref[which, plane] for plane in planes], axis=1)
        right = jnp.concatenate(split(data / blurred), axis=0)
        along_y = stack(dot(lyb_ref[which], right))
        along_x = sides(dot(beside(cut(along_y, count)), xb_ref[which]))
        for i, plane in enumerate(planes):
            s_ref[which, pl.ds(pl.multiple_of(plane * s_stride, 8), rows)] = along_x[i * rows:(i + 1) * rows]


def back_rows(base, count, lzb_ref, s_ref, product_ref):
    outer = lzb_ref.shape[2] // 2
    stride = s_ref.shape[1] // outer
    both = []
    for which in range(2):
        right = stacked([s_ref[which, pl.ds(base + i, outer, stride=stride)] for i in range(count)])
        both.append(stack(dot(lzb_ref[which], right)))
    for i, piece in enumerate(cut(both[0] * both[1], count)):
        product_ref[base + i] = piece


def whole_kernel(blocks, strip_rows, data_hbm, start_hbm, table_hbm, index_ref,
                 all_ref,
                 sbuf, dbuf, table_ref, ts_ref, td_ref, kern_ref, est_ref, est2_ref, data_ref,
                 lz_ref, x_ref, ly_ref, lyb_ref, xb_ref, lzb_ref, t_ref, s_ref,
                 product_ref, other_ref, other2_ref,
                 load_sem, kern_s, kern_r, e_s, e_r, d_s, d_r, h_s, h_r,
                 p_s, p_r, y_s, y_r, z_s, z_r, q_s, q_r, f_s, f_r, g_s, g_r, o_s, o_r, w_s, w_r):
    here = Place(blocks)
    planes, width_x, width_y = start_hbm.shape
    taps = table_ref.shape[2]
    reach = taps - 1
    pad = reach // 2
    depth = 2 * planes
    rows = strip_rows
    wide = rows + 2 * reach
    tall = rows + 2 * pad
    stride = ts_ref.shape[0] // (width_y + 2 * reach)
    half = wide // 2
    k, a, b, c, strip = here.k, here.a, here.b, here.c, here.strip
    below, above = k > 0, k < blocks - 1
    unless = lambda condition: pl.when(jnp.logical_not(condition))
    pieces = planes // pad
    loads = []
    for i, (source, target) in enumerate(((start_hbm, sbuf), (data_hbm, dbuf))):
        for piece in range(pieces):
            at = pl.ds(pad * piece, pad)
            load = pltpu.make_async_copy(source.at[at], target.at[at], load_sem.at[pieces * i + piece])
            load.start()
            loads.append(load)
    load_table = pltpu.make_async_copy(table_hbm, table_ref, load_sem.at[2 * pieces])
    load_table.start()
    ts3 = ts_ref.reshape(width_y + 2 * reach, stride, width_x)
    greet(here)

    ts_ref[pl.ds(0, reach * stride)] = jnp.zeros((reach * stride, width_x), jnp.float32)
    ts_ref[pl.ds((width_y + reach) * stride, reach * stride)] = jnp.zeros((reach * stride, width_x), jnp.float32)
    mine = pl.multiple_of(reach + planes * b, 8)
    theirs = pl.multiple_of(reach + planes * (1 - b), 8)
    rows_c = pl.ds(half * c, half)
    e_copies = []
    for piece in range(pieces):
        loads[piece].wait()

        @pl.loop(0, pad, unroll=4)
        def _(z):
            ts_ref[pl.ds(reach * stride + pad * piece + z, width_y, stride=stride)] = sbuf[pad * piece + z].T

        e_copy = remote(
            ts3.at[pl.ds(rows * here.strip_of(a, 1 - b) + half * c, half), pl.ds(pad * piece, pad)],
            est_ref.at[rows_c, pl.ds(mine + pad * piece, pad)], (e_s, e_r), 6 + piece, here.device(b=1 - b),
        )
        e_copy.start()
        e_copies.append(e_copy)

    load_table.wait()
    table = table_ref[...]
    chosen = lax.broadcasted_iota(jnp.int32, table.shape, 1) == index_ref[0]
    kern = jnp.sum(jnp.where(chosen, table, 0.0), axis=1)
    kern = kern / jnp.sum(kern, axis=-1, keepdims=True)
    kern_ref[a] = jnp.zeros(kern_ref.shape[1:], jnp.float32)
    kern_ref[a, pl.ds(0, 3), pl.ds(0, taps)] = kern
    kern_copy = remote(kern_ref.at[a], kern_ref.at[a], (kern_s, kern_r), 0, here.device(a=1 - a))
    kern_copy.start()

    for z in range(planes):
        td_ref[z, pl.ds(0, pad)] = jnp.zeros((pad, width_x), jnp.float32)
        td_ref[z, pl.ds(pad + width_y, pad)] = jnp.zeros((pad, width_x), jnp.float32)
    for load in loads[pieces:]:
        load.wait()

    @pl.loop(0, planes, unroll=4)
    def _(z):
        td_ref[z, pl.ds(pad, width_y)] = dbuf[z].T

    d_copies = []
    for part, (first, size) in enumerate(((b * (planes - pad), pad), ((1 - b) * pad, planes - pad))):
        for kind, (oa, ob) in enumerate(here.others()):
            copy = remote(
                td_ref.at[pl.ds(first, size), pl.ds(rows * here.strip_of(oa, ob), tall)],
                data_ref.at[a, pl.ds(pad + planes * b + first, size)],
                (d_s, d_r), 3 * part + kind, here.device(a=oa, b=ob),
            )
            copy.start()
            d_copies.append(copy)

    @pl.loop(0, wide, unroll=8)
    def _(row):
        est_ref[row, pl.ds(mine, planes)] = ts3[rows * strip + row, pl.ds(0, planes)]

    @pl.loop(0, planes, unroll=2)
    def _(z):
        data_ref[a, pad + planes * b + z] = td_ref[z, pl.ds(pl.multiple_of(rows * strip, 8), tall)]

    def zero(ref, first_row, count, first, size):
        @pl.loop(0, count, unroll=8)
        def _(row):
            ref[first_row + row, pl.ds(first, size)] = jnp.zeros((size, width_x), jnp.float32)

    unless(below)(lambda: zero(est_ref, 0, wide, 0, reach))
    unless(above)(lambda: zero(est_ref, 0, wide, reach + depth, reach))

    def halo(kind, oa, ob):
        to = k + 2 * ob - 1
        source = k + 1 - 2 * ob
        place = (1 - ob) * (depth + pad)
        copy = remote(
            data_ref.at[oa, pl.ds(pad + ob * (depth - pad), pad)], data_ref.at[oa, pl.ds(place, pad)],
            (h_s, h_r), kind, here.device(k=to),
        )
        sends = (to >= 0) & (to < blocks)
        gets = (source >= 0) & (source < blocks)
        unless(gets)(lambda: zero(data_ref.at[oa], place, pad, 0, tall))
        pl.when(sends)(copy.start)
        return copy, sends, gets

    halos = [halo(3, a, b)]

    kern_copy.wait()
    write_matrices(kern_ref, taps, (lz_ref, x_ref, ly_ref, lyb_ref, xb_ref, lzb_ref))

    for copy in e_copies:
        copy.wait()
    relay = remote(
        est_ref.at[rows_c, pl.ds(theirs, planes)], est_ref.at[rows_c, pl.ds(theirs, planes)],
        (e_s, e_r), 1, here.partner(),
    )
    bottom, top = pl.ds(0, reach), pl.ds(reach + depth, reach)
    first, last = pl.ds(reach, reach), pl.ds(depth, reach)
    up = remote(est_ref.at[rows_c, last], est_ref.at[rows_c, bottom], (e_s, e_r), 2, here.device(k=k + 1))
    down = remote(est_ref.at[rows_c, first], est_ref.at[rows_c, top], (e_s, e_r), 3, here.device(k=k - 1))
    from_below = remote(est_ref.at[rows_c, bottom], est_ref.at[rows_c, bottom], (e_s, e_r), 4, here.partner())
    from_above = remote(est_ref.at[rows_c, top], est_ref.at[rows_c, top], (e_s, e_r), 5, here.partner())
    pl.when(above)(up.start)
    pl.when(below)(down.start)
    relay.start()

    @pl.when(below)
    def _():
        up.wait_recv()
        from_below.start()

    @pl.when(above)
    def _():
        down.wait_recv()
        from_above.start()

    pl.when(above)(up.wait_send)
    pl.when(below)(down.wait_send)
    relay.wait()
    pl.when(below)(from_below.wait)
    pl.when(above)(from_above.wait)

    @pl.loop(0, wide // GROUP)
    def _(step):
        forward_rows(step * GROUP, GROUP, est_ref, lz_ref, x_ref, t_ref)

    def back_planes(base, other):
        ratio_planes(
            [base + i for i in range(pad)] + [other + i for i in range(pad)],
            data_ref, ly_ref, lyb_ref, xb_ref, t_ref, s_ref,
        )

    steps = planes // pad + 1
    for kind, (oa, ob) in enumerate(here.others()):
        d_copies[kind].wait_recv()
        halos.append(halo(kind, oa, ob))

    @pl.loop(0, steps)
    def _(step):
        @pl.when(step == 1)
        def _():
            for copy in d_copies[3:]:
                copy.wait_recv()

        @pl.when(step == steps - 1)
        def _():
            for copy, sends, gets in halos:
                pl.when(gets)(copy.wait_recv)

        outside, edge = step == steps - 1, step == 0
        back_planes(
            jnp.where(outside, 0, jnp.where(edge, pad, 2 * pad * step)),
            jnp.where(outside, depth + pad, jnp.where(edge, depth, 2 * pad * step + pad)),
        )

    chunks = rows // reach
    inside = pl.ds(reach, depth)
    left, right = strip > 0, strip < 3

    def chunk_of(i):
        middle = jnp.where(i == 0, 1, jnp.where(i == 1, chunks, i))
        return jnp.where(i == chunks, 0, jnp.where(i == chunks + 1, chunks + 1, middle))

    def swap(q):
        at = pl.ds(reach * q, reach)
        return remote(product_ref.at[at], other_ref.at[at], (p_s, p_r), q, here.partner())

    @pl.loop(0, chunks)
    def _(i):
        q = chunk_of(i) - 1
        back_rows(reach * q, reach, lzb_ref, s_ref, product_ref)
        swap(q).start()

    unless(left)(lambda: zero(est2_ref, 0, reach, 0, depth + 2 * reach))
    unless(right)(lambda: zero(est2_ref, reach + rows, reach, 0, depth + 2 * reach))
    unless(below)(lambda: zero(est2_ref, 0, wide, 0, reach))
    unless(above)(lambda: zero(est2_ref, 0, wide, reach + depth, reach))

    to_left = remote(
        est2_ref.at[pl.ds(reach, reach), inside], est2_ref.at[pl.ds(reach + rows, reach), inside],
        (y_s, y_r), 0, here.of_strip(strip - 1),
    )
    to_right = remote(
        est2_ref.at[pl.ds(rows, reach), inside], est2_ref.at[pl.ds(0, reach), inside],
        (y_s, y_r), 1, here.of_strip(strip + 1),
    )
    to_block = k + 1 - 2 * c
    z_sends = (to_block >= 0) & (to_block < blocks)
    z_gets = (k - 1 + 2 * c >= 0) & (k - 1 + 2 * c < blocks)
    q_gets = (k + 1 - 2 * c >= 0) & (k + 1 - 2 * c < blocks)
    z_from = pl.multiple_of(reach + (1 - c) * (depth - reach), 8)
    z_to = pl.multiple_of(c * (reach + depth), 8)

    def along_z(e):
        at = pl.ds(reach * e, reach)
        return remote(
            est2_ref.at[at, pl.ds(z_from, reach)], est2_ref.at[at, pl.ds(z_to, reach)],
            (z_s, z_r), e, here.device(k=to_block),
        )

    def across(e):
        at = pl.ds(reach * e, reach)
        return remote(
            est2_ref.at[at, pl.ds(z_to, reach)], est2_ref.at[at, pl.ds(z_to, reach)],
            (q_s, q_r), e, here.partner(),
        )

    @pl.loop(0, chunks)
    def _(i):
        e = chunk_of(i)
        q = e - 1
        swap(q).wait_recv()

        @pl.loop(0, reach, unroll=4)
        def _(r):
            row = reach * q + r
            factor = root(product_ref[row] * other_ref[row])
            est2_ref[reach + row, inside] = est_ref[reach + row, inside] * factor

        pl.when((i == 0) & left)(to_left.start)
        pl.when((i == 1) & right)(to_right.start)
        pl.when(z_sends)(along_z(e).start)

    zone = pl.ds(z_to, reach)
    corner_left = remote(
        est2_ref.at[pl.ds(reach, reach), zone], est2_ref.at[pl.ds(reach + rows, reach), zone],
        (y_s, y_r), 2, here.of_strip(strip - 1),
    )
    corner_right = remote(
        est2_ref.at[pl.ds(rows, reach), zone], est2_ref.at[pl.ds(0, reach), zone],
        (y_s, y_r), 3, here.of_strip(strip + 1),
    )

    def exists(e):
        return ((e > 0) | left) & ((e < chunks + 1) | right)

    @pl.loop(0, chunks + 3)
    def _(i):
        e = chunk_of(i)

        @pl.when((i < chunks) & z_gets)
        def _():
            along_z(e).wait_recv()
            pl.when((i == 0) & left)(corner_left.start)
            pl.when((i == 1) & right)(corner_right.start)

        pl.when((i == chunks) & z_gets & left)(corner_right.wait_recv)
        pl.when((i == chunks + 1) & z_gets & right)(corner_left.wait_recv)
        pl.when((i < chunks + 2) & z_gets & exists(e))(across(e).start)

        @pl.when(i == chunks + 1)
        def _():
            pl.when(left)(to_right.wait_recv)
            pl.when(right)(to_left.wait_recv)

        @pl.when(i >= 1)
        def _():
            before = chunk_of(i - 1)
            pl.when(q_gets & exists(before))(across(before).wait_recv)
            forward_rows(reach * before, reach, est2_ref, lz_ref, x_ref, t_ref)

    @pl.loop(0, chunks)
    def _(q):
        swap(q).wait_send()

    @pl.loop(0, steps)
    def _(step):
        back_planes(2 * pad * step, 2 * pad * step + pad)

    part = reach // 2

    def last_swap(q):
        at = pl.ds(reach * q + part * (1 - c), part)
        return remote(product_ref.at[at], other2_ref.at[at], (f_s, f_r), q, here.partner())

    def gather(q, kind, oa, ob):
        return remote(
            other2_ref.at[pl.ds(reach * q + part * c, part), pl.ds(pl.multiple_of(planes * ob, 8), planes)],
            all_ref.at[pl.ds(rows * strip + reach * q + part * c, part)],
            (g_s, g_r), 3 * q + kind, here.device(a=oa, b=ob),
        )

    def own(q):
        return remote(
            other2_ref.at[pl.ds(reach * q + part * c, part), pl.ds(pl.multiple_of(planes * b, 8), planes)],
            all_ref.at[pl.ds(rows * strip + reach * q + part * c, part)],
            (o_s, o_r), q, here.partner(),
        )

    def onward(q, kind, oa, ob):
        at = pl.ds(rows * here.strip_of(oa, ob) + reach * q + part * c, part)
        return remote(all_ref.at[at], all_ref.at[at], (w_s, w_r), 3 * q + kind, here.partner())

    @pl.loop(0, chunks)
    def _(q):
        back_rows(reach * q, reach, lzb_ref, s_ref, product_ref)
        last_swap(q).start()

    @pl.loop(0, chunks)
    def _(q):
        last_swap(q).wait_recv()

        @pl.loop(0, part, unroll=4)
        def _(r):
            row = reach * q + part * c + r
            factor = root(product_ref[row] * other2_ref[row])
            other2_ref[row] = est2_ref[reach + row, inside] * factor
            all_ref[rows * strip + row] = other2_ref[row, pl.ds(pl.multiple_of(planes * b, 8), planes)]

        for kind in (2, 0, 1):
            gather(q, kind, *here.others()[kind]).start()
        own(q).start()

    @pl.loop(0, chunks)
    def _(q):
        for kind in range(3):
            gather(q, kind, *here.others()[kind]).wait_recv()
            onward(q, kind, *here.others()[kind]).start()

    @pl.loop(0, chunks)
    def _(q):
        last_swap(q).wait_send()
        own(q).wait()
        for kind in range(3):
            gather(q, kind, *here.others()[kind]).wait_send()
            onward(q, kind, *here.others()[kind]).wait()

    for copy in d_copies:
        copy.wait_send()
    for copy, sends, gets in halos:
        pl.when(sends)(copy.wait_send)
    pl.when(left)(to_left.wait_send)
    pl.when(right)(to_right.wait_send)

    pl.when(left & z_gets)(corner_left.wait_send)
    pl.when(right & z_gets)(corner_right.wait_send)

    @pl.loop(0, chunks + 2)
    def _(e):
        pl.when((e > 0) & (e < chunks + 1) & z_sends)(along_z(e).wait_send)
        pl.when(z_gets & exists(e))(across(e).wait_send)


def output_kernel(all_ref, out_ref):
    group, lanes, width = out_ref.shape
    stride = all_ref.shape[0] // width
    base = pl.program_id(0) * group
    for i in range(group):
        out_ref[i] = all_ref[pl.ds(base + i, width, stride=stride)].T


def on_device(blocks, views_data, start, psf_table, psf_index):
    f32, bf16 = jnp.float32, jnp.bfloat16
    planes, width_x, width_y = start.shape
    reach = psf_table.shape[2] - 1
    pad = reach // 2
    rows = width_y // 4
    depth = 2 * planes
    wide, deep = rows + 2 * reach, depth + 2 * reach
    tall, outer = rows + 2 * pad, depth + 2 * pad
    chunks = rows // reach
    dma = lambda n: [pltpu.SemaphoreType.DMA((n,)), pltpu.SemaphoreType.DMA((n,))]

    by_row = jnp.transpose(psf_table, (1, 0, 2))
    gathered = pl.pallas_call(
        functools.partial(whole_kernel, blocks, rows),
        out_shape=jax.ShapeDtypeStruct((width_y, planes, width_x), f32),
        in_specs=[HBM, HBM, HBM, pl.BlockSpec(memory_space=pltpu.SMEM)],
        out_specs=VMEM,
        scratch_shapes=[
            pltpu.VMEM(start.shape, f32),
            pltpu.VMEM(start.shape, f32),
            pltpu.VMEM(by_row.shape, f32),
            pltpu.VMEM(((width_y + 2 * reach) * odd_stride(planes), width_x), f32),
            pltpu.VMEM((planes, width_y + 2 * pad, width_x), f32),
            pltpu.VMEM((2, 8, 128), f32),
            pltpu.VMEM((wide, deep, width_x), f32),
            pltpu.VMEM((wide, deep, width_x), f32),
            pltpu.VMEM((2, outer, tall, width_x), f32),
            pltpu.VMEM((2, 2 * outer, 2 * deep), bf16),
            pltpu.VMEM((2, 2 * width_x, 2 * width_x), bf16),
            pltpu.VMEM((2, 2 * tall, 2 * wide), bf16),
            pltpu.VMEM((2, 2 * rows, 2 * tall), bf16),
            pltpu.VMEM((2, 2 * width_x, 2 * width_x), bf16),
            pltpu.VMEM((2, 2 * depth, 2 * outer), bf16),
            pltpu.VMEM((2, wide * odd_stride(outer), width_x), f32),
            pltpu.VMEM((2, outer * odd_stride(rows), width_x), f32),
            pltpu.VMEM((rows, depth, width_x), f32),
            pltpu.VMEM((rows, depth, width_x), f32),
            pltpu.VMEM((rows, depth, width_x), f32),
            pltpu.SemaphoreType.DMA((2 * (planes // pad) + 1,)),
            *dma(1), *dma(6 + planes // pad), *dma(6), *dma(4),
            *dma(chunks), *dma(4), *dma(chunks + 2), *dma(chunks + 2),
            *dma(chunks), *dma(3 * chunks), *dma(chunks), *dma(3 * chunks),
        ],
        compiler_params=pltpu.CompilerParams(
            collective_id=0, has_side_effects=True, vmem_limit_bytes=VMEM_LIMIT * MIB
        ),
    )(views_data[0], start, by_row, psf_index)
    return pl.pallas_call(
        output_kernel,
        grid=(planes // 4,),
        out_shape=jax.ShapeDtypeStruct(start.shape, f32),
        in_specs=[VMEM],
        out_specs=pl.BlockSpec((4, width_x, width_y), lambda i: (i, 0, 0)),
        compiler_params=pltpu.CompilerParams(vmem_limit_bytes=12 * MIB),
    )(gathered.reshape(width_y * planes, width_x))


def solution(mesh):
    return jax.shard_map(
        functools.partial(on_device, mesh.shape["gz"] // 2),
        mesh=mesh,
        in_specs=(P("view", "gz", None, None), P("gz", None, None), P(), P("view")),
        out_specs=P("gz", None, None),
        check_vma=False,
    )
```

```python
import functools
import jax
import jax.numpy as jnp
from jax import lax
from jax.experimental import pallas as pl
from jax.experimental.pallas import tpu as pltpu
from jax.sharding import PartitionSpec as P

ITERS = 2
GROUP = 32
MESH = pl.DeviceIdType.MESH
VMEM = pl.BlockSpec(memory_space=pltpu.VMEM)
HBM = pl.BlockSpec(memory_space=pltpu.HBM)
VMEM_LIMIT = 48
MIB = 1024 * 1024


def split(value):
    high = value.astype(jnp.bfloat16)
    return high, (value - high.astype(jnp.float32)).astype(jnp.bfloat16)


def dot(lhs, rhs):
    return jnp.dot(lhs, rhs, preferred_element_type=jnp.float32)


def odd_stride(rows):
    return rows + 8 if (rows // 8) % 2 == 0 else rows


class Place:
    def __init__(self, blocks):
        view, gz = lax.axis_index("view"), lax.axis_index("gz")
        self.blocks = blocks
        self.a, self.c = view // 2, view % 2
        self.k, self.b = gz // 2, gz % 2
        self.strip = self.strip_of(self.a, self.b)

    @staticmethod
    def strip_of(a, b):
        return 2 * a + (a + b) % 2

    def device(self, a=None, c=None, k=None, b=None):
        a = self.a if a is None else a
        c = self.c if c is None else c
        k = self.k if k is None else k
        b = self.b if b is None else b
        return (2 * a + c, 2 * k + b)

    def of_strip(self, strip):
        return self.device(a=strip // 2, b=(strip % 2 + strip // 2) % 2)

    def partner(self):
        return self.device(c=1 - self.c)

    def others(self):
        a, b = self.a, self.b
        return ((a, 1 - b), (1 - a, b), (1 - a, 1 - b))


def remote(src, dst, sems, index, device):
    send, recv = sems
    return pltpu.make_async_remote_copy(
        src_ref=src, dst_ref=dst, send_sem=send.at[index], recv_sem=recv.at[index],
        device_id=device, device_id_type=MESH,
    )


def greet(here):
    barrier = pltpu.get_barrier_semaphore()

    def signal(device):
        pl.semaphore_signal(barrier, inc=1, device_id=device, device_id_type=MESH)

    signal(here.partner())
    count = 1
    for a, b in here.others():
        signal(here.device(a=a, b=b))
        count += 1
    for step in (-1, 1):
        there = here.k + step
        inside = (there >= 0) & (there < here.blocks)
        pl.when(inside)(functools.partial(lambda there: signal(here.device(k=there)), there))
        count = count + inside.astype(jnp.int32)
    pl.semaphore_wait(barrier, count)


def band(taps, outputs, inputs, sign, shift):
    at = sign * (
        lax.broadcasted_iota(jnp.int32, (outputs, inputs), 1)
        - lax.broadcasted_iota(jnp.int32, (outputs, inputs), 0)
    ) + shift
    total = jnp.zeros((outputs, inputs), jnp.float32)
    for tap, value in enumerate(taps):
        total = jnp.where(at == tap, value, total)
    return total


def write_left(ref, index, matrix):
    high, low = split(matrix)
    rows, depth = matrix.shape
    top = jnp.concatenate([high, high], axis=1)
    bottom = jnp.concatenate([low, low], axis=1)
    ref[index] = jnp.concatenate([top, bottom], axis=0)


def write_right(ref, index, matrix):
    high, low = split(matrix)
    half = jnp.concatenate([high, low], axis=1)
    ref[index] = jnp.concatenate([half, half], axis=0)


def write_matrices(kern_ref, taps, refs):
    lz_ref, x_ref, ly_ref, lyb_ref, xb_ref, lzb_ref = refs
    reach = taps - 1
    pad = reach // 2
    for which in range(2):
        rows = kern_ref[which]
        kz, kx, ky = ([rows[r:r + 1, t:t + 1] for t in range(taps)] for r in range(3))
        outputs, inputs = lz_ref.shape[1] // 2, lz_ref.shape[2] // 2
        write_left(lz_ref, which, band(kz, outputs, inputs, 1, 0))
        write_right(x_ref, which, band(kx, x_ref.shape[1] // 2, x_ref.shape[2] // 2, -1, pad))
        write_left(ly_ref, which, band(ky, ly_ref.shape[1] // 2, ly_ref.shape[2] // 2, 1, 0))
        write_left(lyb_ref, which, band(ky, lyb_ref.shape[1] // 2, lyb_ref.shape[2] // 2, -1, reach))
        write_right(xb_ref, which, band(kx, xb_ref.shape[1] // 2, xb_ref.shape[2] // 2, 1, pad))
        write_left(lzb_ref, which, band(kz, lzb_ref.shape[1] // 2, lzb_ref.shape[2] // 2, -1, reach))


def sides(product):
    half = product.shape[1] // 2
    return product[:, :half] + product[:, half:]


def stack(product):
    half = product.shape[0] // 2
    return product[:half] + product[half:]


def cut(value, count):
    lanes = value.shape[1] // count
    return [value[:, i * lanes:(i + 1) * lanes] for i in range(count)]


def stacked(values):
    return jnp.concatenate([jnp.concatenate(split(value), axis=0) for value in values], axis=1)


def beside(pieces):
    return jnp.concatenate(split(jnp.concatenate(pieces, axis=0)), axis=1)


def root(value):
    return jnp.sqrt(jnp.sqrt(value))


def forward_rows(base, count, est_ref, lz_ref, x_ref, t_ref):
    outer = lz_ref.shape[1] // 2
    half = t_ref.shape[0] // 2
    stride = half // est_ref.shape[0]
    left = lz_ref[...].reshape(4 * outer, lz_ref.shape[2])
    both = dot(left, stacked([est_ref[base + i] for i in range(count)]))
    for which in range(2):
        along_z = stack(both[2 * outer * which:2 * outer * (which + 1)])
        along_x = sides(dot(beside(cut(along_z, count)), x_ref[which]))
        for i in range(count):
            at = pl.multiple_of(half * which + (base + i) * stride, 8)
            t_ref[pl.ds(at, outer)] = along_x[i * outer:(i + 1) * outer]


def ratio_planes(row, planes, wide, data_ref, ly_ref, lyb_ref, xb_ref, t_ref, s_ref):
    count = len(planes)
    reads, tall, rows = ly_ref.shape[2] // 2, ly_ref.shape[1] // 2, lyb_ref.shape[1] // 2
    half = t_ref.shape[0] // 2
    t_stride = half // wide
    s_stride = s_ref.shape[1] // data_ref.shape[1]
    for which in range(2):
        first = half * which + row * t_stride
        right = stacked([t_ref[pl.ds(first + plane, reads, stride=t_stride)] for plane in planes])
        blurred = stack(dot(ly_ref[which], right))
        data = jnp.concatenate([data_ref[which, plane, pl.ds(row, tall)] for plane in planes], axis=1)
        right = jnp.concatenate(split(data / blurred), axis=0)
        along_y = stack(dot(lyb_ref[which], right))
        along_x = sides(dot(beside(cut(along_y, count)), xb_ref[which]))
        for i, plane in enumerate(planes):
            at = pl.multiple_of(plane * s_stride + row, 8)
            s_ref[which, pl.ds(at, rows)] = along_x[i * rows:(i + 1) * rows]


def back_rows(base, count, lzb_ref, s_ref, product_ref):
    outer = lzb_ref.shape[2] // 2
    stride = s_ref.shape[1] // outer
    both = []
    for which in range(2):
        right = stacked([s_ref[which, pl.ds(base + i, outer, stride=stride)] for i in range(count)])
        both.append(stack(dot(lzb_ref[which], right)))
    for i, piece in enumerate(cut(both[0] * both[1], count)):
        product_ref[base + i] = piece


def whole_kernel(blocks, strip_rows, data_hbm, start_hbm, table_hbm, index_ref,
                 all_ref,
                 sbuf, table_ref, td_ref, kern_ref, est_ref, est2_ref, data_ref,
                 lz_ref, x_ref, ly_ref, lyb_ref, xb_ref, lzb_ref, t_ref, t2_ref, s_ref,
                 product_ref, other_ref, other2_ref,
                 load_sem, kern_s, kern_r, e_s, e_r, d_s, d_r, h_s, h_r,
                 p_s, p_r, y_s, y_r, z_s, z_r, q_s, q_r, f_s, f_r, g_s, g_r, o_s, o_r, w_s, w_r):
    here = Place(blocks)
    planes, width_x, width_y = start_hbm.shape
    taps = table_ref.shape[2]
    reach = taps - 1
    pad = reach // 2
    depth = 2 * planes
    rows = strip_rows
    wide = rows + 2 * reach
    tall = rows + 2 * pad
    stride = odd_stride(planes)
    half = wide // 2
    k, a, b, c, strip = here.k, here.a, here.b, here.c, here.strip
    below, above = k > 0, k < blocks - 1
    unless = lambda condition: pl.when(jnp.logical_not(condition))
    pieces = planes // pad

    def load(source, index, piece):
        at = pl.ds(pad * piece, pad)
        copy = pltpu.make_async_copy(source.at[at], sbuf.at[at], load_sem.at[pieces * index + piece])
        copy.start()
        return copy

    loads = [load(start_hbm, 0, piece) for piece in range(pieces)]
    ts_ref = t2_ref.at[pl.ds(0, (width_y + 2 * reach) * stride)]
    load_table = pltpu.make_async_copy(table_hbm, table_ref, load_sem.at[2 * pieces])
    load_table.start()
    ts3 = ts_ref.reshape(width_y + 2 * reach, stride, width_x)
    greet(here)

    ts_ref[pl.ds(0, reach * stride)] = jnp.zeros((reach * stride, width_x), jnp.float32)
    ts_ref[pl.ds((width_y + reach) * stride, reach * stride)] = jnp.zeros((reach * stride, width_x), jnp.float32)
    mine = pl.multiple_of(reach + planes * b, 8)
    theirs = pl.multiple_of(reach + planes * (1 - b), 8)
    rows_c = pl.ds(half * c, half)
    e_copies = []
    for piece in range(pieces):
        loads[piece].wait()

        @pl.loop(0, pad, unroll=4)
        def _(z):
            ts_ref[pl.ds(reach * stride + pad * piece + z, width_y, stride=stride)] = sbuf[pad * piece + z].T

        e_copy = remote(
            ts3.at[pl.ds(rows * here.strip_of(a, 1 - b) + half * c, half), pl.ds(pad * piece, pad)],
            est_ref.at[rows_c, pl.ds(mine + pad * piece, pad)], (e_s, e_r), 6 + piece, here.device(b=1 - b),
        )
        e_copy.start()
        e_copies.append(e_copy)
        loads.append(load(data_hbm, 1, piece))

    load_table.wait()
    table = table_ref[...]
    chosen = lax.broadcasted_iota(jnp.int32, table.shape, 1) == index_ref[0]
    kern = jnp.sum(jnp.where(chosen, table, 0.0), axis=1)
    kern = kern / jnp.sum(kern, axis=-1, keepdims=True)
    kern_ref[a] = jnp.zeros(kern_ref.shape[1:], jnp.float32)
    kern_ref[a, pl.ds(0, 3), pl.ds(0, taps)] = kern
    kern_copy = remote(kern_ref.at[a], kern_ref.at[a], (kern_s, kern_r), 0, here.device(a=1 - a))
    kern_copy.start()

    for z in range(planes):
        td_ref[z, pl.ds(0, pad)] = jnp.zeros((pad, width_x), jnp.float32)
        td_ref[z, pl.ds(pad + width_y, pad)] = jnp.zeros((pad, width_x), jnp.float32)
    for load in loads[pieces:]:
        load.wait()

    @pl.loop(0, planes, unroll=4)
    def _(z):
        td_ref[z, pl.ds(pad, width_y)] = sbuf[z].T

    size = 2 * reach
    parts = rows // size
    chunks = rows // reach
    ascends = lambda strip: strip % 2 == 0

    def new_rows(part, strip):
        first = size * part + (2 * pad if part else 0)
        count = size if part else size + 2 * pad
        return pl.ds(pl.multiple_of(jnp.where(ascends(strip), first, tall - first - count), 8), count)

    def data_copy(part, inner, kind):
        oa, ob = here.others()[kind]
        first, count = ((1 - b) * pad, planes - pad) if inner else (b * (planes - pad), pad)
        target = here.strip_of(oa, ob)
        at = new_rows(part, target)
        return remote(
            td_ref.at[pl.ds(first, count), pl.ds(pl.multiple_of(rows * target + at.start, 8), at.size)],
            data_ref.at[a, pl.ds(pad + planes * b + first, count), at],
            (d_s, d_r), (2 * part + inner) * 3 + kind, here.device(a=oa, b=ob),
        )

    every_data = [(part, inner, kind) for part in range(parts) for inner in range(2) for kind in (2, 0, 1)]
    for which in every_data:
        data_copy(*which).start()

    @pl.loop(0, wide, unroll=8)
    def _(row):
        est_ref[row, pl.ds(mine, planes)] = ts3[rows * strip + row, pl.ds(0, planes)]

    @pl.loop(0, planes, unroll=2)
    def _(z):
        data_ref[a, pad + planes * b + z] = td_ref[z, pl.ds(pl.multiple_of(rows * strip, 8), tall)]

    def zero(ref, first_row, count, first, size):
        @pl.loop(0, count, unroll=8)
        def _(row):
            ref[first_row + row, pl.ds(first, size)] = jnp.zeros((size, width_x), jnp.float32)

    unless(below)(lambda: zero(est_ref, 0, wide, 0, reach))
    unless(above)(lambda: zero(est_ref, 0, wide, reach + depth, reach))

    quad = (*here.others(), (a, b))

    def halo_goes(kind):
        to = k + 2 * quad[kind][1] - 1
        return (to >= 0) & (to < blocks)

    def halo_comes(kind):
        source = k + 1 - 2 * quad[kind][1]
        return (source >= 0) & (source < blocks)

    def halo_copy(part, kind):
        oa, ob = quad[kind]
        at = new_rows(part, strip)
        return remote(
            data_ref.at[oa, pl.ds(pad + ob * (depth - pad), pad), at],
            data_ref.at[oa, pl.ds((1 - ob) * (depth + pad), pad), at],
            (h_s, h_r), 4 * part + kind, here.device(k=k + 2 * ob - 1),
        )

    for kind, (oa, ob) in enumerate(quad):
        unless(halo_comes(kind))(functools.partial(zero, data_ref.at[oa], (1 - ob) * (depth + pad), pad, 0, tall))
    for part in range(parts):
        pl.when(halo_goes(3))(halo_copy(part, 3).start)

    def edges_come(part):
        for kind in (0, 1, 2):
            data_copy(part, 0, kind).wait_recv()
            pl.when(halo_goes(kind))(halo_copy(part, kind).start)

    def rest_comes(part):
        for kind in (0, 1, 2):
            data_copy(part, 1, kind).wait_recv()
        for kind in range(4):
            pl.when(halo_comes(kind))(halo_copy(part, kind).wait_recv)

    kern_copy.wait()
    write_matrices(kern_ref, taps, (lz_ref, x_ref, ly_ref, lyb_ref, xb_ref, lzb_ref))

    for copy in e_copies:
        copy.wait()
    relay = remote(
        est_ref.at[rows_c, pl.ds(theirs, planes)], est_ref.at[rows_c, pl.ds(theirs, planes)],
        (e_s, e_r), 1, here.partner(),
    )
    bottom, top = pl.ds(0, reach), pl.ds(reach + depth, reach)
    first, last = pl.ds(reach, reach), pl.ds(depth, reach)
    up = remote(est_ref.at[rows_c, last], est_ref.at[rows_c, bottom], (e_s, e_r), 2, here.device(k=k + 1))
    down = remote(est_ref.at[rows_c, first], est_ref.at[rows_c, top], (e_s, e_r), 3, here.device(k=k - 1))
    from_below = remote(est_ref.at[rows_c, bottom], est_ref.at[rows_c, bottom], (e_s, e_r), 4, here.partner())
    from_above = remote(est_ref.at[rows_c, top], est_ref.at[rows_c, top], (e_s, e_r), 5, here.partner())
    pl.when(above)(up.start)
    pl.when(below)(down.start)
    relay.start()
    edges_come(0)

    @pl.when(below)
    def _():
        up.wait_recv()
        from_below.start()

    @pl.when(above)
    def _():
        down.wait_recv()
        from_above.start()

    pl.when(above)(up.wait_send)
    pl.when(below)(down.wait_send)
    relay.wait()
    pl.when(below)(from_below.wait)
    pl.when(above)(from_above.wait)

    left, right = strip > 0, strip < 3

    @pl.loop(0, wide // GROUP)
    def _(step):
        forward_rows(step * GROUP, GROUP, est_ref, lz_ref, x_ref, t_ref)

    chunk_of = lambda i: jnp.where(ascends(strip), i, chunks + 1 - i)
    row_of = lambda i: pl.multiple_of(reach * (chunk_of(i) - 1), reach)
    inside = pl.ds(reach, depth)
    step_first = jnp.where(ascends(strip), -1, 1)
    strip_first, strip_last = strip + step_first, strip - step_first
    has_first = (strip_first >= 0) & (strip_first < 4)
    has_last = (strip_last >= 0) & (strip_last < 4)

    def ratio_part(part, from_ref):
        row = pl.multiple_of(size * jnp.where(ascends(strip), part, parts - 1 - part), size)

        @pl.loop(0, (depth + 2 * pad) // (2 * pad))
        def _(step):
            ratio_planes(
                row, [2 * pad * step + i for i in range(2 * pad)], wide,
                data_ref, ly_ref, lyb_ref, xb_ref, from_ref, s_ref,
            )

    def places(part, body):
        pl.loop(1 + 2 * part, 3 + 2 * part)(body)

    def swap(i):
        at = pl.ds(row_of(i), reach)
        return remote(product_ref.at[at], other_ref.at[at], (p_s, p_r), i, here.partner())

    to_block = k + 1 - 2 * c
    z_sends = (to_block >= 0) & (to_block < blocks)
    z_gets = (k - 1 + 2 * c >= 0) & (k - 1 + 2 * c < blocks)
    q_gets = (k + 1 - 2 * c >= 0) & (k + 1 - 2 * c < blocks)
    z_from = pl.multiple_of(reach + (1 - c) * (depth - reach), 8)
    z_to = pl.multiple_of(c * (reach + depth), 8)

    def along_z(i):
        at = pl.ds(reach + row_of(i), reach)
        return remote(
            est2_ref.at[at, pl.ds(z_from, reach)], est2_ref.at[at, pl.ds(z_to, reach)],
            (z_s, z_r), i, here.device(k=to_block),
        )

    def across(i):
        at = pl.ds(reach + row_of(i), reach)
        return remote(
            est2_ref.at[at, pl.ds(z_to, reach)], est2_ref.at[at, pl.ds(z_to, reach)],
            (q_s, q_r), i, here.partner(),
        )

    def to_strip(last, zone, index):
        place = chunks if last else 1
        return remote(
            est2_ref.at[pl.ds(reach + row_of(place), reach), zone],
            est2_ref.at[pl.ds(pl.multiple_of(
                jnp.where(ascends(strip) == bool(last), 0, reach + rows), reach), reach), zone],
            (y_s, y_r), index, here.of_strip(strip_last if last else strip_first),
        )

    def y_main(last):
        return to_strip(last, inside, last)

    def y_corner(last):
        return to_strip(last, pl.ds(z_to, reach), 2 + last)

    unless(left)(lambda: zero(est2_ref, 0, reach, 0, depth + 2 * reach))
    unless(right)(lambda: zero(est2_ref, reach + rows, reach, 0, depth + 2 * reach))
    unless(below)(lambda: zero(est2_ref, 0, wide, 0, reach))
    unless(above)(lambda: zero(est2_ref, 0, wide, reach + depth, reach))

    def first_update(part):
        ratio_part(part, t_ref)

        def make(i):
            back_rows(row_of(i), reach, lzb_ref, s_ref, product_ref)
            swap(i).start()

        def use(i):
            swap(i).wait_recv()

            @pl.loop(0, reach, unroll=4)
            def _(r):
                row = row_of(i) + r
                factor = root(product_ref[row] * other_ref[row])
                est2_ref[reach + row, inside] = est_ref[reach + row, inside] * factor

            pl.when(z_sends)(along_z(i).start)
            pl.when((i == 1) & has_first)(y_main(0).start)
            pl.when((i == chunks) & has_last)(y_main(1).start)

        places(part, make)
        places(part, use)

    def arrive(i):
        @pl.when(z_gets)
        def _():
            along_z(i).wait_recv()
            pl.when((i == 1) & has_first)(y_corner(0).start)
            pl.when((i == chunks) & has_last)(y_corner(1).start)
            across(i).start()

    def arrive_side(last, there):
        @pl.when(there)
        def _():
            y_main(last).wait_recv()

            @pl.when(z_gets)
            def _():
                y_corner(last).wait_recv()
                across((chunks + 1) * last).start()

    def forward(i):
        there = ((i > 0) | has_first) & ((i < chunks + 1) | has_last)
        pl.when(q_gets & there)(across(i).wait_recv)
        forward_rows(pl.multiple_of(reach * chunk_of(i), reach), reach, est2_ref, lz_ref, x_ref, t2_ref)

    half_rows = reach // 2

    def last_swap(i):
        at = pl.ds(row_of(i) + half_rows * (1 - c), half_rows)
        return remote(product_ref.at[at], other2_ref.at[at], (f_s, f_r), i, here.partner())

    def gather(i, kind):
        oa, ob = here.others()[kind]
        return remote(
            other2_ref.at[pl.ds(row_of(i) + half_rows * c, half_rows), pl.ds(pl.multiple_of(planes * ob, 8), planes)],
            all_ref.at[pl.ds(rows * strip + row_of(i) + half_rows * c, half_rows)],
            (g_s, g_r), 3 * i + kind, here.device(a=oa, b=ob),
        )

    def own(i):
        return remote(
            other2_ref.at[pl.ds(row_of(i) + half_rows * c, half_rows), pl.ds(pl.multiple_of(planes * b, 8), planes)],
            all_ref.at[pl.ds(rows * strip + row_of(i) + half_rows * c, half_rows)],
            (o_s, o_r), i, here.partner(),
        )

    def onward(i, kind):
        theirs = here.strip_of(*here.others()[kind])
        chunk = jnp.where(ascends(theirs), i - 1, chunks - i)
        at = pl.ds(rows * theirs + reach * chunk + half_rows * c, half_rows)
        return remote(all_ref.at[at], all_ref.at[at], (w_s, w_r), 3 * i + kind, here.partner())

    def last_update(part):
        ratio_part(part, t2_ref)

        def make(i):
            swap(i).wait_send()
            back_rows(row_of(i), reach, lzb_ref, s_ref, product_ref)
            last_swap(i).start()

        def use(i):
            last_swap(i).wait_recv()

            @pl.loop(0, half_rows, unroll=4)
            def _(r):
                row = row_of(i) + half_rows * c + r
                factor = root(product_ref[row] * other2_ref[row])
                other2_ref[row] = est2_ref[reach + row, inside] * factor
                all_ref[rows * strip + row] = other2_ref[row, pl.ds(pl.multiple_of(planes * b, 8), planes)]

            for kind in (2, 0, 1):
                gather(i, kind).start()
            own(i).start()

        places(part, make)
        places(part, use)

    for part in range(parts - 1):
        edges_come(part + 1)
        rest_comes(part)
        first_update(part)
    early = 2 * (parts - 1) - 1
    pl.loop(1, early)(arrive)
    pl.loop(1, early)(forward)
    rest_comes(parts - 1)
    first_update(parts - 1)
    pl.loop(early, chunks - 1)(arrive)
    arrive_side(0, has_first)
    forward(0)
    pl.loop(early, chunks - 1)(forward)
    for part in range(parts - 2):
        last_update(part)
    pl.loop(chunks - 1, chunks + 1)(arrive)
    pl.loop(chunks - 1, chunks + 1)(forward)
    last_update(parts - 2)
    arrive_side(1, has_last)
    forward(chunks + 1)
    last_update(parts - 1)

    @pl.loop(1, chunks + 1)
    def _(i):
        for kind in range(3):
            gather(i, kind).wait_recv()
            onward(i, kind).start()

    @pl.loop(1, chunks + 1)
    def _(i):
        last_swap(i).wait_send()
        own(i).wait()
        for kind in range(3):
            gather(i, kind).wait_send()
            onward(i, kind).wait()
        pl.when(z_sends)(along_z(i).wait_send)

    for which in every_data:
        data_copy(*which).wait_send()
    for part in range(parts):
        for kind in range(4):
            pl.when(halo_goes(kind))(halo_copy(part, kind).wait_send)
    for last, there in enumerate((has_first, has_last)):
        pl.when(there)(y_main(last).wait_send)
        pl.when(there & z_gets)(y_corner(last).wait_send)

    @pl.loop(0, chunks + 2)
    def _(i):
        there = ((i > 0) | has_first) & ((i < chunks + 1) | has_last)
        pl.when(z_gets & there)(across(i).wait_send)


def output_kernel(all_ref, out_ref):
    group, lanes, width = out_ref.shape
    stride = all_ref.shape[0] // width
    base = pl.program_id(0) * group
    for i in range(group):
        out_ref[i] = all_ref[pl.ds(base + i, width, stride=stride)].T


def on_device(blocks, views_data, start, psf_table, psf_index):
    f32, bf16 = jnp.float32, jnp.bfloat16
    planes, width_x, width_y = start.shape
    reach = psf_table.shape[2] - 1
    pad = reach // 2
    rows = width_y // 4
    depth = 2 * planes
    wide, deep = rows + 2 * reach, depth + 2 * reach
    tall, outer = rows + 2 * pad, depth + 2 * pad
    chunks = rows // reach
    size = 2 * reach
    parts = rows // size
    dma = lambda n: [pltpu.SemaphoreType.DMA((n,)), pltpu.SemaphoreType.DMA((n,))]

    by_row = jnp.transpose(psf_table, (1, 0, 2))
    gathered = pl.pallas_call(
        functools.partial(whole_kernel, blocks, rows),
        out_shape=jax.ShapeDtypeStruct((width_y, planes, width_x), f32),
        in_specs=[HBM, HBM, HBM, pl.BlockSpec(memory_space=pltpu.SMEM)],
        out_specs=VMEM,
        scratch_shapes=[
            pltpu.VMEM(start.shape, f32),
            pltpu.VMEM(by_row.shape, f32),
            pltpu.VMEM((planes, width_y + 2 * pad, width_x), f32),
            pltpu.VMEM((2, 8, 128), f32),
            pltpu.VMEM((wide, deep, width_x), f32),
            pltpu.VMEM((wide, deep, width_x), f32),
            pltpu.VMEM((2, outer, tall, width_x), f32),
            pltpu.VMEM((2, 2 * outer, 2 * deep), bf16),
            pltpu.VMEM((2, 2 * width_x, 2 * width_x), bf16),
            pltpu.VMEM((2, 2 * (size + 2 * pad), 2 * (size + 2 * reach)), bf16),
            pltpu.VMEM((2, 2 * size, 2 * (size + 2 * pad)), bf16),
            pltpu.VMEM((2, 2 * width_x, 2 * width_x), bf16),
            pltpu.VMEM((2, 2 * depth, 2 * outer), bf16),
            pltpu.VMEM((2 * wide * odd_stride(outer), width_x), f32),
            pltpu.VMEM((2 * wide * odd_stride(outer), width_x), f32),
            pltpu.VMEM((2, outer * odd_stride(rows), width_x), f32),
            pltpu.VMEM((rows, depth, width_x), f32),
            pltpu.VMEM((rows, depth, width_x), f32),
            pltpu.VMEM((rows, depth, width_x), f32),
            pltpu.SemaphoreType.DMA((2 * (planes // pad) + 1,)),
            *dma(1), *dma(6 + planes // pad), *dma(6 * parts), *dma(4 * parts),
            *dma(chunks + 1), *dma(4), *dma(chunks + 2), *dma(chunks + 2),
            *dma(chunks + 1), *dma(3 * chunks + 3), *dma(chunks + 1), *dma(3 * chunks + 3),
        ],
        compiler_params=pltpu.CompilerParams(
            collective_id=0, has_side_effects=True, vmem_limit_bytes=VMEM_LIMIT * MIB
        ),
    )(views_data[0], start, by_row, psf_index)
    return pl.pallas_call(
        output_kernel,
        grid=(planes // 4,),
        out_shape=jax.ShapeDtypeStruct(start.shape, f32),
        in_specs=[VMEM],
        out_specs=pl.BlockSpec((4, width_x, width_y), lambda i: (i, 0, 0)),
        compiler_params=pltpu.CompilerParams(vmem_limit_bytes=12 * MIB),
    )(gathered.reshape(width_y * planes, width_x))


def solution(mesh):
    return jax.shard_map(
        functools.partial(on_device, mesh.shape["gz"] // 2),
        mesh=mesh,
        in_specs=(P("view", "gz", None, None), P("gz", None, None), P(), P("view")),
        out_specs=P("gz", None, None),
        check_vma=False,
    )
```

```python
import functools
import jax
import jax.numpy as jnp
from jax import lax
from jax.experimental import pallas as pl
from jax.experimental.pallas import tpu as pltpu
from jax.sharding import PartitionSpec as P

ITERS = 2
GROUP = 32
MESH = pl.DeviceIdType.MESH
VMEM = pl.BlockSpec(memory_space=pltpu.VMEM)
HBM = pl.BlockSpec(memory_space=pltpu.HBM)
VMEM_LIMIT = 48
MIB = 1024 * 1024


def split(value):
    high = value.astype(jnp.bfloat16)
    return high, (value - high.astype(jnp.float32)).astype(jnp.bfloat16)


def dot(lhs, rhs):
    return jnp.dot(lhs, rhs, preferred_element_type=jnp.float32)


def odd_stride(rows):
    return rows + 8 if (rows // 8) % 2 == 0 else rows


class Place:
    def __init__(self, blocks):
        view, gz = lax.axis_index("view"), lax.axis_index("gz")
        self.blocks = blocks
        self.a, self.c = view // 2, view % 2
        self.k, self.b = gz // 2, gz % 2
        self.strip = self.strip_of(self.a, self.b)

    @staticmethod
    def strip_of(a, b):
        return 2 * a + (a + b) % 2

    def device(self, a=None, c=None, k=None, b=None):
        a = self.a if a is None else a
        c = self.c if c is None else c
        k = self.k if k is None else k
        b = self.b if b is None else b
        return (2 * a + c, 2 * k + b)

    def of_strip(self, strip):
        return self.device(a=strip // 2, b=(strip % 2 + strip // 2) % 2)

    def partner(self):
        return self.device(c=1 - self.c)

    def others(self):
        a, b = self.a, self.b
        return ((a, 1 - b), (1 - a, b), (1 - a, 1 - b))


def remote(src, dst, sems, index, device):
    send, recv = sems
    return pltpu.make_async_remote_copy(
        src_ref=src, dst_ref=dst, send_sem=send.at[index], recv_sem=recv.at[index],
        device_id=device, device_id_type=MESH,
    )


def greet(here):
    barrier = pltpu.get_barrier_semaphore()

    def signal(device):
        pl.semaphore_signal(barrier, inc=1, device_id=device, device_id_type=MESH)

    signal(here.partner())
    count = 1
    for a, b in here.others():
        signal(here.device(a=a, b=b))
        count += 1
    for step in (-1, 1):
        there = here.k + step
        inside = (there >= 0) & (there < here.blocks)
        pl.when(inside)(functools.partial(lambda there: signal(here.device(k=there)), there))
        count = count + inside.astype(jnp.int32)
    pl.semaphore_wait(barrier, count)


def band(taps, outputs, inputs, sign, shift):
    at = sign * (
        lax.broadcasted_iota(jnp.int32, (outputs, inputs), 1)
        - lax.broadcasted_iota(jnp.int32, (outputs, inputs), 0)
    ) + shift
    total = jnp.zeros((outputs, inputs), jnp.float32)
    for tap, value in enumerate(taps):
        total = jnp.where(at == tap, value, total)
    return total


def write_left(ref, index, matrix):
    high, low = split(matrix)
    rows, depth = matrix.shape
    top = jnp.concatenate([high, high], axis=1)
    bottom = jnp.concatenate([low, low], axis=1)
    ref[index] = jnp.concatenate([top, bottom], axis=0)


def write_right(ref, index, matrix):
    high, low = split(matrix)
    half = jnp.concatenate([high, low], axis=1)
    ref[index] = jnp.concatenate([half, half], axis=0)


def write_matrices(kern_ref, taps, refs):
    lz_ref, x_ref, ly_ref, lyb_ref, xb_ref, lzb_ref = refs
    reach = taps - 1
    pad = reach // 2
    for which in range(2):
        rows = kern_ref[which]
        kz, kx, ky = ([rows[r:r + 1, t:t + 1] for t in range(taps)] for r in range(3))
        outputs, inputs = lz_ref.shape[1] // 2, lz_ref.shape[2] // 2
        write_left(lz_ref, which, band(kz, outputs, inputs, 1, 0))
        write_right(x_ref, which, band(kx, x_ref.shape[1] // 2, x_ref.shape[2] // 2, -1, pad))
        write_left(ly_ref, which, band(ky, ly_ref.shape[1] // 2, ly_ref.shape[2] // 2, 1, 0))
        write_left(lyb_ref, which, band(ky, lyb_ref.shape[1] // 2, lyb_ref.shape[2] // 2, -1, reach))
        write_right(xb_ref, which, band(kx, xb_ref.shape[1] // 2, xb_ref.shape[2] // 2, 1, pad))
        write_left(lzb_ref, which, band(kz, lzb_ref.shape[1] // 2, lzb_ref.shape[2] // 2, -1, reach))


def sides(product):
    half = product.shape[1] // 2
    return product[:, :half] + product[:, half:]


def stack(product):
    half = product.shape[0] // 2
    return product[:half] + product[half:]


def cut(value, count):
    lanes = value.shape[1] // count
    return [value[:, i * lanes:(i + 1) * lanes] for i in range(count)]


def stacked(values):
    return jnp.concatenate([jnp.concatenate(split(value), axis=0) for value in values], axis=1)


def beside(pieces):
    return jnp.concatenate(split(jnp.concatenate(pieces, axis=0)), axis=1)


def root(value):
    return jnp.sqrt(jnp.sqrt(value))


def forward_rows(base, count, est_ref, lz_ref, x_ref, t_ref):
    outer = lz_ref.shape[1] // 2
    half = t_ref.shape[0] // 2
    stride = half // est_ref.shape[0]
    left = lz_ref[...].reshape(4 * outer, lz_ref.shape[2])
    both = dot(left, stacked([est_ref[base + i] for i in range(count)]))
    for which in range(2):
        along_z = stack(both[2 * outer * which:2 * outer * (which + 1)])
        along_x = sides(dot(beside(cut(along_z, count)), x_ref[which]))
        for i in range(count):
            at = pl.multiple_of(half * which + (base + i) * stride, 8)
            t_ref[pl.ds(at, outer)] = along_x[i * outer:(i + 1) * outer]


def ratio_planes(row, planes, wide, data_ref, ly_ref, lyb_ref, xb_ref, t_ref, s_ref):
    count = len(planes)
    reads, tall, rows = ly_ref.shape[2] // 2, ly_ref.shape[1] // 2, lyb_ref.shape[1] // 2
    half = t_ref.shape[0] // 2
    t_stride = half // wide
    s_stride = s_ref.shape[1] // data_ref.shape[1]
    for which in range(2):
        first = half * which + row * t_stride
        right = stacked([t_ref[pl.ds(first + plane, reads, stride=t_stride)] for plane in planes])
        blurred = stack(dot(ly_ref[which], right))
        data = jnp.concatenate([data_ref[which, plane, pl.ds(row, tall)] for plane in planes], axis=1)
        right = jnp.concatenate(split(data / blurred), axis=0)
        along_y = stack(dot(lyb_ref[which], right))
        along_x = sides(dot(beside(cut(along_y, count)), xb_ref[which]))
        for i, plane in enumerate(planes):
            at = pl.multiple_of(plane * s_stride + row, 8)
            s_ref[which, pl.ds(at, rows)] = along_x[i * rows:(i + 1) * rows]


def back_rows(base, count, lzb_ref, s_ref, product_ref):
    outer = lzb_ref.shape[2] // 2
    stride = s_ref.shape[1] // outer
    both = []
    for which in range(2):
        right = stacked([s_ref[which, pl.ds(base + i, outer, stride=stride)] for i in range(count)])
        both.append(stack(dot(lzb_ref[which], right)))
    for i, piece in enumerate(cut(both[0] * both[1], count)):
        product_ref[base + i] = piece


def whole_kernel(blocks, strip_rows, data_hbm, start_hbm, table_hbm, index_ref,
                 all_ref,
                 sbuf, table_ref, td_ref, kern_ref, est_ref, est2_ref, data_ref,
                 lz_ref, x_ref, ly_ref, lyb_ref, xb_ref, lzb_ref, t_ref, t2_ref, s_ref,
                 product_ref, other_ref, other2_ref,
                 load_sem, kern_s, kern_r, e_s, e_r, d_s, d_r, h_s, h_r,
                 p_s, p_r, y_s, y_r, z_s, z_r, q_s, q_r, f_s, f_r, g_s, g_r, o_s, o_r, w_s, w_r):
    here = Place(blocks)
    planes, width_x, width_y = start_hbm.shape
    taps = table_ref.shape[2]
    reach = taps - 1
    pad = reach // 2
    depth = 2 * planes
    rows = strip_rows
    wide = rows + 2 * reach
    tall = rows + 2 * pad
    stride = odd_stride(planes)
    half = wide // 2
    k, a, b, c, strip = here.k, here.a, here.b, here.c, here.strip
    below, above = k > 0, k < blocks - 1
    unless = lambda condition: pl.when(jnp.logical_not(condition))
    pieces = planes // pad

    def load(source, index, piece):
        at = pl.ds(pad * piece, pad)
        copy = pltpu.make_async_copy(source.at[at], sbuf.at[at], load_sem.at[pieces * index + piece])
        copy.start()
        return copy

    loads = [load(start_hbm, 0, piece) for piece in range(pieces)]
    ts_ref = t2_ref.at[pl.ds(0, (width_y + 2 * reach) * stride)]
    load_table = pltpu.make_async_copy(table_hbm, table_ref, load_sem.at[2 * pieces])
    load_table.start()
    ts3 = ts_ref.reshape(width_y + 2 * reach, stride, width_x)
    greet(here)

    ts_ref[pl.ds(0, reach * stride)] = jnp.zeros((reach * stride, width_x), jnp.float32)
    ts_ref[pl.ds((width_y + reach) * stride, reach * stride)] = jnp.zeros((reach * stride, width_x), jnp.float32)
    mine = pl.multiple_of(reach + planes * b, 8)
    theirs = pl.multiple_of(reach + planes * (1 - b), 8)
    rows_c = pl.ds(half * c, half)
    e_copies = []
    for piece in range(pieces):
        loads[piece].wait()

        @pl.loop(0, pad, unroll=4)
        def _(z):
            ts_ref[pl.ds(reach * stride + pad * piece + z, width_y, stride=stride)] = sbuf[pad * piece + z].T

        e_copy = remote(
            ts3.at[pl.ds(rows * here.strip_of(a, 1 - b) + half * c, half), pl.ds(pad * piece, pad)],
            est_ref.at[rows_c, pl.ds(mine + pad * piece, pad)], (e_s, e_r), 6 + piece, here.device(b=1 - b),
        )
        e_copy.start()
        e_copies.append(e_copy)
        loads.append(load(data_hbm, 1, piece))

    load_table.wait()
    table = table_ref[...]
    chosen = lax.broadcasted_iota(jnp.int32, table.shape, 1) == index_ref[0]
    kern = jnp.sum(jnp.where(chosen, table, 0.0), axis=1)
    kern = kern / jnp.sum(kern, axis=-1, keepdims=True)
    kern_ref[a] = jnp.zeros(kern_ref.shape[1:], jnp.float32)
    kern_ref[a, pl.ds(0, 3), pl.ds(0, taps)] = kern
    kern_copy = remote(kern_ref.at[a], kern_ref.at[a], (kern_s, kern_r), 0, here.device(a=1 - a))
    kern_copy.start()

    for z in range(planes):
        td_ref[z, pl.ds(0, pad)] = jnp.zeros((pad, width_x), jnp.float32)
        td_ref[z, pl.ds(pad + width_y, pad)] = jnp.zeros((pad, width_x), jnp.float32)
    for load in loads[pieces:]:
        load.wait()

    @pl.loop(0, planes, unroll=4)
    def _(z):
        td_ref[z, pl.ds(pad, width_y)] = sbuf[z].T

    size = 2 * reach
    parts = rows // size
    chunks = rows // reach
    ascends = lambda strip: strip % 2 == 0

    def new_rows(part, strip):
        first = size * part + (2 * pad if part else 0)
        count = size if part else size + 2 * pad
        return pl.ds(pl.multiple_of(jnp.where(ascends(strip), first, tall - first - count), 8), count)

    def data_copy(part, inner, kind):
        oa, ob = here.others()[kind]
        first, count = ((1 - b) * pad, planes - pad) if inner else (b * (planes - pad), pad)
        target = here.strip_of(oa, ob)
        at = new_rows(part, target)
        return remote(
            td_ref.at[pl.ds(first, count), pl.ds(pl.multiple_of(rows * target + at.start, 8), at.size)],
            data_ref.at[a, pl.ds(pad + planes * b + first, count), at],
            (d_s, d_r), (2 * part + inner) * 3 + kind, here.device(a=oa, b=ob),
        )

    every_data = [(part, inner, kind) for inner in range(2) for part in range(parts) for kind in (2, 0, 1)]
    for which in every_data:
        data_copy(*which).start()

    @pl.loop(0, wide, unroll=8)
    def _(row):
        est_ref[row, pl.ds(mine, planes)] = ts3[rows * strip + row, pl.ds(0, planes)]

    @pl.loop(0, planes, unroll=2)
    def _(z):
        data_ref[a, pad + planes * b + z] = td_ref[z, pl.ds(pl.multiple_of(rows * strip, 8), tall)]

    def zero(ref, first_row, count, first, size):
        @pl.loop(0, count, unroll=8)
        def _(row):
            ref[first_row + row, pl.ds(first, size)] = jnp.zeros((size, width_x), jnp.float32)

    unless(below)(lambda: zero(est_ref, 0, wide, 0, reach))
    unless(above)(lambda: zero(est_ref, 0, wide, reach + depth, reach))

    quad = (*here.others(), (a, b))

    def halo_goes(kind):
        to = k + 2 * quad[kind][1] - 1
        return (to >= 0) & (to < blocks)

    def halo_comes(kind):
        source = k + 1 - 2 * quad[kind][1]
        return (source >= 0) & (source < blocks)

    def halo_copy(part, kind):
        oa, ob = quad[kind]
        at = new_rows(part, strip)
        return remote(
            data_ref.at[oa, pl.ds(pad + ob * (depth - pad), pad), at],
            data_ref.at[oa, pl.ds((1 - ob) * (depth + pad), pad), at],
            (h_s, h_r), 4 * part + kind, here.device(k=k + 2 * ob - 1),
        )

    for kind, (oa, ob) in enumerate(quad):
        unless(halo_comes(kind))(functools.partial(zero, data_ref.at[oa], (1 - ob) * (depth + pad), pad, 0, tall))
    for part in range(parts):
        pl.when(halo_goes(3))(halo_copy(part, 3).start)

    def edges_come(part):
        for kind in (0, 1, 2):
            data_copy(part, 0, kind).wait_recv()
            pl.when(halo_goes(kind))(halo_copy(part, kind).start)

    def rest_comes(part):
        for kind in (0, 1, 2):
            data_copy(part, 1, kind).wait_recv()
        for kind in range(4):
            pl.when(halo_comes(kind))(halo_copy(part, kind).wait_recv)

    kern_copy.wait()
    write_matrices(kern_ref, taps, (lz_ref, x_ref, ly_ref, lyb_ref, xb_ref, lzb_ref))

    for copy in e_copies:
        copy.wait()
    relay = remote(
        est_ref.at[rows_c, pl.ds(theirs, planes)], est_ref.at[rows_c, pl.ds(theirs, planes)],
        (e_s, e_r), 1, here.partner(),
    )
    bottom, top = pl.ds(0, reach), pl.ds(reach + depth, reach)
    first, last = pl.ds(reach, reach), pl.ds(depth, reach)
    up = remote(est_ref.at[rows_c, last], est_ref.at[rows_c, bottom], (e_s, e_r), 2, here.device(k=k + 1))
    down = remote(est_ref.at[rows_c, first], est_ref.at[rows_c, top], (e_s, e_r), 3, here.device(k=k - 1))
    from_below = remote(est_ref.at[rows_c, bottom], est_ref.at[rows_c, bottom], (e_s, e_r), 4, here.partner())
    from_above = remote(est_ref.at[rows_c, top], est_ref.at[rows_c, top], (e_s, e_r), 5, here.partner())
    pl.when(above)(up.start)
    pl.when(below)(down.start)
    relay.start()
    edges_come(0)

    @pl.when(below)
    def _():
        up.wait_recv()
        from_below.start()

    @pl.when(above)
    def _():
        down.wait_recv()
        from_above.start()

    edges_come(1)
    pl.when(above)(up.wait_send)
    pl.when(below)(down.wait_send)
    relay.wait()
    pl.when(below)(from_below.wait)
    pl.when(above)(from_above.wait)
    left, right = strip > 0, strip < 3

    @pl.loop(0, wide // GROUP)
    def _(step):
        forward_rows(step * GROUP, GROUP, est_ref, lz_ref, x_ref, t_ref)

    chunk_of = lambda i: jnp.where(ascends(strip), i, chunks + 1 - i)
    row_of = lambda i: pl.multiple_of(reach * (chunk_of(i) - 1), reach)
    inside = pl.ds(reach, depth)
    step_first = jnp.where(ascends(strip), -1, 1)
    strip_first, strip_last = strip + step_first, strip - step_first
    has_first = (strip_first >= 0) & (strip_first < 4)
    has_last = (strip_last >= 0) & (strip_last < 4)

    def ratio_part(part, from_ref):
        row = pl.multiple_of(size * jnp.where(ascends(strip), part, parts - 1 - part), size)

        ratio_planes(
            row, range(depth + 2 * pad), wide, data_ref, ly_ref, lyb_ref, xb_ref, from_ref, s_ref,
        )

    def places(part, body):
        pl.loop(1 + 2 * part, 3 + 2 * part)(body)

    def swap(i):
        at = pl.ds(row_of(i), reach)
        return remote(product_ref.at[at], other_ref.at[at], (p_s, p_r), i, here.partner())

    to_block = k + 1 - 2 * c
    z_sends = (to_block >= 0) & (to_block < blocks)
    z_gets = (k - 1 + 2 * c >= 0) & (k - 1 + 2 * c < blocks)
    q_gets = (k + 1 - 2 * c >= 0) & (k + 1 - 2 * c < blocks)
    z_from = pl.multiple_of(reach + (1 - c) * (depth - reach), 8)
    z_to = pl.multiple_of(c * (reach + depth), 8)

    def along_z(i):
        at = pl.ds(reach + row_of(i), reach)
        return remote(
            est2_ref.at[at, pl.ds(z_from, reach)], est2_ref.at[at, pl.ds(z_to, reach)],
            (z_s, z_r), i, here.device(k=to_block),
        )

    def across(i):
        at = pl.ds(reach + row_of(i), reach)
        return remote(
            est2_ref.at[at, pl.ds(z_to, reach)], est2_ref.at[at, pl.ds(z_to, reach)],
            (q_s, q_r), i, here.partner(),
        )

    def to_strip(last, zone, index):
        place = chunks if last else 1
        return remote(
            est2_ref.at[pl.ds(reach + row_of(place), reach), zone],
            est2_ref.at[pl.ds(pl.multiple_of(
                jnp.where(ascends(strip) == bool(last), 0, reach + rows), reach), reach), zone],
            (y_s, y_r), index, here.of_strip(strip_last if last else strip_first),
        )

    def y_main(last):
        return to_strip(last, pl.ds(pl.multiple_of(reach + planes * c, 8), planes), last)

    def y_across(last):
        at = pl.ds(reach + row_of((chunks + 1) * last), reach)
        zone = pl.ds(pl.multiple_of(reach + planes * c, 8), planes)
        return remote(
            est2_ref.at[at, zone], est2_ref.at[at, zone], (q_s, q_r), chunks + 2 + last, here.partner(),
        )

    def y_corner(last):
        return to_strip(last, pl.ds(z_to, reach), 2 + last)

    unless(left)(lambda: zero(est2_ref, 0, reach, 0, depth + 2 * reach))
    unless(right)(lambda: zero(est2_ref, reach + rows, reach, 0, depth + 2 * reach))
    unless(below)(lambda: zero(est2_ref, 0, wide, 0, reach))
    unless(above)(lambda: zero(est2_ref, 0, wide, reach + depth, reach))

    def first_update(part):
        ratio_part(part, t_ref)

        def make(i):
            back_rows(row_of(i), reach, lzb_ref, s_ref, product_ref)
            swap(i).start()

        def use(i):
            swap(i).wait_recv()

            @pl.loop(0, reach, unroll=4)
            def _(r):
                row = row_of(i) + r
                factor = root(product_ref[row] * other_ref[row])
                est2_ref[reach + row, inside] = est_ref[reach + row, inside] * factor

            pl.when(z_sends)(along_z(i).start)
            pl.when((i == 1) & has_first)(y_main(0).start)
            pl.when((i == chunks) & has_last)(y_main(1).start)

        places(part, make)
        places(part, use)

    def arrive(i):
        @pl.when(z_gets)
        def _():
            along_z(i).wait_recv()
            pl.when((i == 1) & has_first)(y_corner(0).start)
            pl.when((i == chunks) & has_last)(y_corner(1).start)
            across(i).start()

    def arrive_side(last, there):
        @pl.when(there)
        def _():
            y_main(last).wait_recv()
            y_across(last).start()

            @pl.when(z_gets)
            def _():
                y_corner(last).wait_recv()
                across((chunks + 1) * last).start()

    def side_forward(last, there):
        pl.when(there)(y_across(last).wait_recv)
        forward((chunks + 1) * last)

    def forward(i):
        there = ((i > 0) | has_first) & ((i < chunks + 1) | has_last)
        pl.when(q_gets & there)(across(i).wait_recv)
        forward_rows(pl.multiple_of(reach * chunk_of(i), reach), reach, est2_ref, lz_ref, x_ref, t2_ref)

    half_rows = reach // 2

    def last_swap(i):
        at = pl.ds(row_of(i) + half_rows * (1 - c), half_rows)
        return remote(product_ref.at[at], other2_ref.at[at], (f_s, f_r), i, here.partner())

    def gather(i, kind):
        oa, ob = here.others()[kind]
        return remote(
            other2_ref.at[pl.ds(row_of(i) + half_rows * c, half_rows), pl.ds(pl.multiple_of(planes * ob, 8), planes)],
            all_ref.at[pl.ds(rows * strip + row_of(i) + half_rows * c, half_rows)],
            (g_s, g_r), 3 * i + kind, here.device(a=oa, b=ob),
        )

    def own(i):
        return remote(
            other2_ref.at[pl.ds(row_of(i) + half_rows * c, half_rows), pl.ds(pl.multiple_of(planes * b, 8), planes)],
            all_ref.at[pl.ds(rows * strip + row_of(i) + half_rows * c, half_rows)],
            (o_s, o_r), i, here.partner(),
        )

    def onward(i, kind):
        theirs = here.strip_of(*here.others()[kind])
        chunk = jnp.where(ascends(theirs), i - 1, chunks - i)
        at = pl.ds(rows * theirs + reach * chunk + half_rows * c, half_rows)
        return remote(all_ref.at[at], all_ref.at[at], (w_s, w_r), 3 * i + kind, here.partner())

    def last_update():

        def make(i):
            swap(i).wait_send()
            back_rows(row_of(i), reach, lzb_ref, s_ref, product_ref)
            last_swap(i).start()

        def use(i):
            last_swap(i).wait_recv()

            @pl.loop(0, half_rows, unroll=4)
            def _(r):
                row = row_of(i) + half_rows * c + r
                factor = root(product_ref[row] * other2_ref[row])
                other2_ref[row] = est2_ref[reach + row, inside] * factor
                all_ref[rows * strip + row] = other2_ref[row, pl.ds(pl.multiple_of(planes * b, 8), planes)]

            for kind in (2, 0, 1):
                gather(i, kind).start()
            own(i).start()

        return make, use

    make, use = last_update()
    for part in range(2, parts):
        edges_come(part)
    early = 2 * (parts - 1) - 1
    for part in range(parts - 1):
        rest_comes(part)
        first_update(part)
    pl.loop(1, early)(arrive)
    pl.loop(1, early)(forward)
    rest_comes(parts - 1)
    first_update(parts - 1)
    pl.loop(early, chunks - 1)(arrive)
    arrive_side(0, has_first)
    pl.loop(early, chunks - 1)(forward)
    side_forward(0, has_first)
    for part in range(parts - 2):
        ratio_part(part, t2_ref)
        places(part, make)
    pl.loop(chunks - 1, chunks + 1)(arrive)
    for part in range(parts - 2):
        places(part, use)
    pl.loop(chunks - 1, chunks + 1)(forward)
    ratio_part(parts - 2, t2_ref)
    places(parts - 2, make)
    arrive_side(1, has_last)
    places(parts - 2, use)
    side_forward(1, has_last)
    ratio_part(parts - 1, t2_ref)
    places(parts - 1, make)
    places(parts - 1, use)

    @pl.loop(1, chunks + 1)
    def _(i):
        for kind in range(3):
            gather(i, kind).wait_recv()
            onward(i, kind).start()

    @pl.loop(1, chunks + 1)
    def _(i):
        last_swap(i).wait_send()
        own(i).wait()
        for kind in range(3):
            gather(i, kind).wait_send()
            onward(i, kind).wait()
        pl.when(z_sends)(along_z(i).wait_send)

    for which in every_data:
        data_copy(*which).wait_send()
    for part in range(parts):
        for kind in range(4):
            pl.when(halo_goes(kind))(halo_copy(part, kind).wait_send)
    for last, there in enumerate((has_first, has_last)):
        pl.when(there)(y_main(last).wait_send)
        pl.when(there)(y_across(last).wait_send)
        pl.when(there & z_gets)(y_corner(last).wait_send)

    @pl.loop(0, chunks + 2)
    def _(i):
        there = ((i > 0) | has_first) & ((i < chunks + 1) | has_last)
        pl.when(z_gets & there)(across(i).wait_send)


def output_kernel(all_ref, out_ref):
    group, lanes, width = out_ref.shape
    stride = all_ref.shape[0] // width
    base = pl.program_id(0) * group
    for i in range(group):
        out_ref[i] = all_ref[pl.ds(base + i, width, stride=stride)].T


def on_device(blocks, views_data, start, psf_table, psf_index):
    f32, bf16 = jnp.float32, jnp.bfloat16
    planes, width_x, width_y = start.shape
    reach = psf_table.shape[2] - 1
    pad = reach // 2
    rows = width_y // 4
    depth = 2 * planes
    wide, deep = rows + 2 * reach, depth + 2 * reach
    tall, outer = rows + 2 * pad, depth + 2 * pad
    chunks = rows // reach
    size = 2 * reach
    parts = rows // size
    dma = lambda n: [pltpu.SemaphoreType.DMA((n,)), pltpu.SemaphoreType.DMA((n,))]

    by_row = jnp.transpose(psf_table, (1, 0, 2))
    gathered = pl.pallas_call(
        functools.partial(whole_kernel, blocks, rows),
        out_shape=jax.ShapeDtypeStruct((width_y, planes, width_x), f32),
        in_specs=[HBM, HBM, HBM, pl.BlockSpec(memory_space=pltpu.SMEM)],
        out_specs=VMEM,
        scratch_shapes=[
            pltpu.VMEM(start.shape, f32),
            pltpu.VMEM(by_row.shape, f32),
            pltpu.VMEM((planes, width_y + 2 * pad, width_x), f32),
            pltpu.VMEM((2, 8, 128), f32),
            pltpu.VMEM((wide, deep, width_x), f32),
            pltpu.VMEM((wide, deep, width_x), f32),
            pltpu.VMEM((2, outer, tall, width_x), f32),
            pltpu.VMEM((2, 2 * outer, 2 * deep), bf16),
            pltpu.VMEM((2, 2 * width_x, 2 * width_x), bf16),
            pltpu.VMEM((2, 2 * (size + 2 * pad), 2 * (size + 2 * reach)), bf16),
            pltpu.VMEM((2, 2 * size, 2 * (size + 2 * pad)), bf16),
            pltpu.VMEM((2, 2 * width_x, 2 * width_x), bf16),
            pltpu.VMEM((2, 2 * depth, 2 * outer), bf16),
            pltpu.VMEM((2 * wide * odd_stride(outer), width_x), f32),
            pltpu.VMEM((2 * wide * odd_stride(outer), width_x), f32),
            pltpu.VMEM((2, outer * odd_stride(rows), width_x), f32),
            pltpu.VMEM((rows, depth, width_x), f32),
            pltpu.VMEM((rows, depth, width_x), f32),
            pltpu.VMEM((rows, depth, width_x), f32),
            pltpu.SemaphoreType.DMA((2 * (planes // pad) + 1,)),
            *dma(1), *dma(6 + planes // pad), *dma(6 * parts), *dma(4 * parts),
            *dma(chunks + 1), *dma(4), *dma(chunks + 1), *dma(chunks + 4),
            *dma(chunks + 1), *dma(3 * chunks + 3), *dma(chunks + 1), *dma(3 * chunks + 3),
        ],
        compiler_params=pltpu.CompilerParams(
            collective_id=0, has_side_effects=True, vmem_limit_bytes=VMEM_LIMIT * MIB
        ),
    )(views_data[0], start, by_row, psf_index)
    return pl.pallas_call(
        output_kernel,
        grid=(planes // 4,),
        out_shape=jax.ShapeDtypeStruct(start.shape, f32),
        in_specs=[VMEM],
        out_specs=pl.BlockSpec((4, width_x, width_y), lambda i: (i, 0, 0)),
        compiler_params=pltpu.CompilerParams(vmem_limit_bytes=12 * MIB),
    )(gathered.reshape(width_y * planes, width_x))


def solution(mesh):
    return jax.shard_map(
        functools.partial(on_device, mesh.shape["gz"] // 2),
        mesh=mesh,
        in_specs=(P("view", "gz", None, None), P("gz", None, None), P(), P("view")),
        out_specs=P("gz", None, None),
        check_vma=False,
    )
```

```python
import functools
import jax
import jax.numpy as jnp
from jax import lax
from jax.experimental import pallas as pl
from jax.experimental.pallas import tpu as pltpu
from jax.sharding import PartitionSpec as P

ITERS = 2
GROUP = 32
MESH = pl.DeviceIdType.MESH
VMEM = pl.BlockSpec(memory_space=pltpu.VMEM)
HBM = pl.BlockSpec(memory_space=pltpu.HBM)
VMEM_LIMIT = 48
SEMAPHORES = 25
MIB = 1024 * 1024


def split(value):
    high = value.astype(jnp.bfloat16)
    return high, (value - high.astype(jnp.float32)).astype(jnp.bfloat16)


def dot(lhs, rhs):
    return jnp.dot(lhs, rhs, preferred_element_type=jnp.float32)


def odd_stride(rows):
    return rows + 8 if (rows // 8) % 2 == 0 else rows


def part_sizes(chunks):
    return (chunks - 4, 2, 2)


class Place:
    def __init__(self, blocks):
        view, gz = lax.axis_index("view"), lax.axis_index("gz")
        self.blocks = blocks
        self.a, self.c = view // 2, view % 2
        self.k, self.b = gz // 2, gz % 2
        self.strip = self.strip_of(self.a, self.b)

    @staticmethod
    def strip_of(a, b):
        return 2 * a + (a + b) % 2

    def device(self, a=None, c=None, k=None, b=None):
        a = self.a if a is None else a
        c = self.c if c is None else c
        k = self.k if k is None else k
        b = self.b if b is None else b
        return (2 * a + c, 2 * k + b)

    def of_strip(self, strip):
        return self.device(a=strip // 2, b=(strip % 2 + strip // 2) % 2)

    def partner(self):
        return self.device(c=1 - self.c)

    def others(self):
        a, b = self.a, self.b
        return ((a, 1 - b), (1 - a, b), (1 - a, 1 - b))


def remote(src, dst, sems, index, device):
    send, recv = sems
    return pltpu.make_async_remote_copy(
        src_ref=src, dst_ref=dst, send_sem=send.at[index], recv_sem=recv.at[index],
        device_id=device, device_id_type=MESH,
    )


def greet(here):
    barrier = pltpu.get_barrier_semaphore()

    def signal(device):
        pl.semaphore_signal(barrier, inc=1, device_id=device, device_id_type=MESH)

    signal(here.partner())
    count = 1
    for a, b in here.others():
        signal(here.device(a=a, b=b))
        count += 1
    for step in (-1, 1):
        there = here.k + step
        inside = (there >= 0) & (there < here.blocks)
        pl.when(inside)(functools.partial(lambda there: signal(here.device(k=there)), there))
        count = count + inside.astype(jnp.int32)
    pl.semaphore_wait(barrier, count)


def band(taps, outputs, inputs, sign, shift):
    at = sign * (
        lax.broadcasted_iota(jnp.int32, (outputs, inputs), 1)
        - lax.broadcasted_iota(jnp.int32, (outputs, inputs), 0)
    ) + shift
    total = jnp.zeros((outputs, inputs), jnp.float32)
    for tap, value in enumerate(taps):
        total = jnp.where(at == tap, value, total)
    return total


def write_left(ref, index, matrix):
    high, low = split(matrix)
    rows, depth = matrix.shape
    top = jnp.concatenate([high, high], axis=1)
    bottom = jnp.concatenate([low, low], axis=1)
    ref[index] = jnp.concatenate([top, bottom], axis=0)


def write_right(ref, index, matrix):
    high, low = split(matrix)
    half = jnp.concatenate([high, low], axis=1)
    ref[index] = jnp.concatenate([half, half], axis=0)


def write_matrices(kern_ref, taps, refs, y_refs):
    lz_ref, x_ref, xb_ref, lzb_ref = refs
    reach = taps - 1
    pad = reach // 2
    for which in range(2):
        rows = kern_ref[which]
        kz, kx, ky = ([rows[r:r + 1, t:t + 1] for t in range(taps)] for r in range(3))
        outputs, inputs = lz_ref.shape[1] // 2, lz_ref.shape[2] // 2
        write_left(lz_ref, which, band(kz, outputs, inputs, 1, 0))
        write_right(x_ref, which, band(kx, x_ref.shape[1] // 2, x_ref.shape[2] // 2, -1, pad))
        for i, ref in enumerate(y_refs):
            write_left(ref, which, band(ky, ref.shape[1] // 2, ref.shape[2] // 2, *((-1, reach) if i % 2 else (1, 0))))
        write_right(xb_ref, which, band(kx, xb_ref.shape[1] // 2, xb_ref.shape[2] // 2, 1, pad))
        write_left(lzb_ref, which, band(kz, lzb_ref.shape[1] // 2, lzb_ref.shape[2] // 2, -1, reach))


def sides(product):
    half = product.shape[1] // 2
    return product[:, :half] + product[:, half:]


def stack(product):
    half = product.shape[0] // 2
    return product[:half] + product[half:]


def cut(value, count):
    lanes = value.shape[1] // count
    return [value[:, i * lanes:(i + 1) * lanes] for i in range(count)]


def stacked(values):
    return jnp.concatenate([jnp.concatenate(split(value), axis=0) for value in values], axis=1)


def beside(pieces):
    return jnp.concatenate(split(jnp.concatenate(pieces, axis=0)), axis=1)


def root(value):
    return jnp.sqrt(jnp.sqrt(value))


def forward_rows(base, count, est_ref, lz_ref, x_ref, t_ref):
    outer = lz_ref.shape[1] // 2
    half = t_ref.shape[0] // 2
    stride = half // est_ref.shape[0]
    left = lz_ref[...].reshape(4 * outer, lz_ref.shape[2])
    both = dot(left, stacked([est_ref[base + i] for i in range(count)]))
    for which in range(2):
        along_z = stack(both[2 * outer * which:2 * outer * (which + 1)])
        along_x = sides(dot(beside(cut(along_z, count)), x_ref[which]))
        for i in range(count):
            at = pl.multiple_of(half * which + (base + i) * stride, 8)
            t_ref[pl.ds(at, outer)] = along_x[i * outer:(i + 1) * outer]


def ratio_planes(row, planes, wide, data_ref, ly_ref, lyb_ref, xb_ref, t_ref, s_ref):
    count = len(planes)
    reads, tall, rows = ly_ref.shape[2] // 2, ly_ref.shape[1] // 2, lyb_ref.shape[1] // 2
    half = t_ref.shape[0] // 2
    t_stride = half // wide
    s_stride = s_ref.shape[1] // data_ref.shape[1]
    for which in range(2):
        first = half * which + row * t_stride
        right = stacked([t_ref[pl.ds(first + plane, reads, stride=t_stride)] for plane in planes])
        blurred = stack(dot(ly_ref[which], right))
        data = jnp.concatenate([data_ref[which, plane, pl.ds(row, tall)] for plane in planes], axis=1)
        right = jnp.concatenate(split(data / blurred), axis=0)
        along_y = stack(dot(lyb_ref[which], right))
        along_x = sides(dot(beside(cut(along_y, count)), xb_ref[which]))
        for i, plane in enumerate(planes):
            at = pl.multiple_of(plane * s_stride + row, 8)
            s_ref[which, pl.ds(at, rows)] = along_x[i * rows:(i + 1) * rows]


def back_rows(base, count, lzb_ref, s_ref, product_ref):
    outer = lzb_ref.shape[2] // 2
    stride = s_ref.shape[1] // outer
    both = []
    for which in range(2):
        right = stacked([s_ref[which, pl.ds(base + i, outer, stride=stride)] for i in range(count)])
        both.append(stack(dot(lzb_ref[which], right)))
    for i, piece in enumerate(cut(both[0] * both[1], count)):
        product_ref[base + i] = piece


def whole_kernel(blocks, strip_rows, data_hbm, start_hbm, table_hbm, index_ref,
                 all_ref,
                 sbuf, table_ref, td_ref, kern_ref, est_ref, est2_ref, data_ref,
                 lz_ref, x_ref, xb_ref, lzb_ref, t_ref, t2_ref, s_ref,
                 product_ref, other_ref, other2_ref, new_ref, *rest):
    y_refs = rest[:-SEMAPHORES]
    (load_sem, kern_s, kern_r, e_s, e_r, d_s, d_r, h_s, h_r,
     p_s, p_r, y_s, y_r, z_s, z_r, q_s, q_r, f_s, f_r, g_s, g_r, o_s, o_r, w_s, w_r) = rest[-SEMAPHORES:]
    here = Place(blocks)
    planes, width_x, width_y = start_hbm.shape
    taps = table_ref.shape[2]
    reach = taps - 1
    pad = reach // 2
    depth = 2 * planes
    rows = strip_rows
    wide = rows + 2 * reach
    tall = rows + 2 * pad
    stride = odd_stride(planes)
    half = wide // 2
    k, a, b, c, strip = here.k, here.a, here.b, here.c, here.strip
    below, above = k > 0, k < blocks - 1
    unless = lambda condition: pl.when(jnp.logical_not(condition))
    pieces = planes // pad

    def load(source, index, piece):
        at = pl.ds(pad * piece, pad)
        copy = pltpu.make_async_copy(source.at[at], sbuf.at[at], load_sem.at[pieces * index + piece])
        copy.start()
        return copy

    loads = [load(start_hbm, 0, piece) for piece in range(pieces)]
    ts_ref = t2_ref.at[pl.ds(0, (width_y + 2 * reach) * stride)]
    load_table = pltpu.make_async_copy(table_hbm, table_ref, load_sem.at[2 * pieces])
    load_table.start()
    ts3 = ts_ref.reshape(width_y + 2 * reach, stride, width_x)
    greet(here)

    ts_ref[pl.ds(0, reach * stride)] = jnp.zeros((reach * stride, width_x), jnp.float32)
    ts_ref[pl.ds((width_y + reach) * stride, reach * stride)] = jnp.zeros((reach * stride, width_x), jnp.float32)
    mine = pl.multiple_of(reach + planes * b, 8)
    theirs = pl.multiple_of(reach + planes * (1 - b), 8)
    rows_c = pl.ds(half * c, half)
    e_copies = []
    for piece in range(pieces):
        loads[piece].wait()

        @pl.loop(0, pad, unroll=4)
        def _(z):
            ts_ref[pl.ds(reach * stride + pad * piece + z, width_y, stride=stride)] = sbuf[pad * piece + z].T

        e_copy = remote(
            ts3.at[pl.ds(rows * here.strip_of(a, 1 - b) + half * c, half), pl.ds(pad * piece, pad)],
            est_ref.at[rows_c, pl.ds(mine + pad * piece, pad)], (e_s, e_r), 6 + piece, here.device(b=1 - b),
        )
        e_copy.start()
        e_copies.append(e_copy)
        loads.append(load(data_hbm, 1, piece))

    load_table.wait()
    table = table_ref[...]
    chosen = lax.broadcasted_iota(jnp.int32, table.shape, 1) == index_ref[0]
    kern = jnp.sum(jnp.where(chosen, table, 0.0), axis=1)
    kern = kern / jnp.sum(kern, axis=-1, keepdims=True)
    kern_ref[a] = jnp.zeros(kern_ref.shape[1:], jnp.float32)
    kern_ref[a, pl.ds(0, 3), pl.ds(0, taps)] = kern
    kern_copy = remote(kern_ref.at[a], kern_ref.at[a], (kern_s, kern_r), 0, here.device(a=1 - a))
    kern_copy.start()

    for z in range(planes):
        td_ref[z, pl.ds(0, pad)] = jnp.zeros((pad, width_x), jnp.float32)
        td_ref[z, pl.ds(pad + width_y, pad)] = jnp.zeros((pad, width_x), jnp.float32)
    for load in loads[pieces:]:
        load.wait()

    @pl.loop(0, planes, unroll=4)
    def _(z):
        td_ref[z, pl.ds(pad, width_y)] = sbuf[z].T

    chunks = rows // reach
    sizes = part_sizes(chunks)
    parts = len(sizes)
    starts = [sum(sizes[:part]) for part in range(parts)]
    ascends = lambda strip: strip % 2 == 0

    def new_rows(part, strip):
        first = reach * starts[part] + (2 * pad if part else 0)
        count = reach * sizes[part] + (0 if part else 2 * pad)
        return pl.ds(pl.multiple_of(jnp.where(ascends(strip), first, tall - first - count), 8), count)

    def data_copy(part, inner, kind):
        oa, ob = here.others()[kind]
        first, count = ((1 - b) * pad, planes - pad) if inner else (b * (planes - pad), pad)
        target = here.strip_of(oa, ob)
        at = new_rows(part, target)
        return remote(
            td_ref.at[pl.ds(first, count), pl.ds(pl.multiple_of(rows * target + at.start, 8), at.size)],
            data_ref.at[a, pl.ds(pad + planes * b + first, count), at],
            (d_s, d_r), (2 * part + inner) * 3 + kind, here.device(a=oa, b=ob),
        )

    every_data = [(part, inner, kind) for inner in range(2) for part in range(parts) for kind in (2, 0, 1)]
    for which in every_data:
        data_copy(*which).start()

    @pl.loop(0, wide, unroll=8)
    def _(row):
        est_ref[row, pl.ds(mine, planes)] = ts3[rows * strip + row, pl.ds(0, planes)]

    @pl.loop(0, planes, unroll=2)
    def _(z):
        data_ref[a, pad + planes * b + z] = td_ref[z, pl.ds(pl.multiple_of(rows * strip, 8), tall)]

    def zero(ref, first_row, count, first, size):
        @pl.loop(0, count, unroll=8)
        def _(row):
            ref[first_row + row, pl.ds(first, size)] = jnp.zeros((size, width_x), jnp.float32)

    unless(below)(lambda: zero(est_ref, 0, wide, 0, reach))
    unless(above)(lambda: zero(est_ref, 0, wide, reach + depth, reach))

    quad = (*here.others(), (a, b))

    def halo_goes(kind):
        to = k + 2 * quad[kind][1] - 1
        return (to >= 0) & (to < blocks)

    def halo_comes(kind):
        source = k + 1 - 2 * quad[kind][1]
        return (source >= 0) & (source < blocks)

    def halo_copy(part, kind):
        oa, ob = quad[kind]
        at = new_rows(part, strip)
        return remote(
            data_ref.at[oa, pl.ds(pad + ob * (depth - pad), pad), at],
            data_ref.at[oa, pl.ds((1 - ob) * (depth + pad), pad), at],
            (h_s, h_r), 4 * part + kind, here.device(k=k + 2 * ob - 1),
        )

    for kind, (oa, ob) in enumerate(quad):
        unless(halo_comes(kind))(functools.partial(zero, data_ref.at[oa], (1 - ob) * (depth + pad), pad, 0, tall))
    for part in range(parts):
        pl.when(halo_goes(3))(halo_copy(part, 3).start)

    def edges_come(part):
        for kind in (0, 1, 2):
            data_copy(part, 0, kind).wait_recv()
            pl.when(halo_goes(kind))(halo_copy(part, kind).start)

    def rest_comes(part):
        for kind in (0, 1, 2):
            data_copy(part, 1, kind).wait_recv()
        for kind in range(4):
            pl.when(halo_comes(kind))(halo_copy(part, kind).wait_recv)

    kern_copy.wait()
    write_matrices(kern_ref, taps, (lz_ref, x_ref, xb_ref, lzb_ref), y_refs)

    for copy in e_copies:
        copy.wait()
    relay = remote(
        est_ref.at[rows_c, pl.ds(theirs, planes)], est_ref.at[rows_c, pl.ds(theirs, planes)],
        (e_s, e_r), 1, here.partner(),
    )
    bottom, top = pl.ds(0, reach), pl.ds(reach + depth, reach)
    first, last = pl.ds(reach, reach), pl.ds(depth, reach)
    up = remote(est_ref.at[rows_c, last], est_ref.at[rows_c, bottom], (e_s, e_r), 2, here.device(k=k + 1))
    down = remote(est_ref.at[rows_c, first], est_ref.at[rows_c, top], (e_s, e_r), 3, here.device(k=k - 1))
    from_below = remote(est_ref.at[rows_c, bottom], est_ref.at[rows_c, bottom], (e_s, e_r), 4, here.partner())
    from_above = remote(est_ref.at[rows_c, top], est_ref.at[rows_c, top], (e_s, e_r), 5, here.partner())
    pl.when(above)(up.start)
    pl.when(below)(down.start)
    relay.start()
    edges_come(0)

    @pl.when(below)
    def _():
        up.wait_recv()
        from_below.start()

    @pl.when(above)
    def _():
        down.wait_recv()
        from_above.start()

    edges_come(1)
    pl.when(above)(up.wait_send)
    pl.when(below)(down.wait_send)
    relay.wait()
    pl.when(below)(from_below.wait)
    pl.when(above)(from_above.wait)
    left, right = strip > 0, strip < 3

    @pl.loop(0, wide // GROUP)
    def _(step):
        forward_rows(step * GROUP, GROUP, est_ref, lz_ref, x_ref, t_ref)

    chunk_of = lambda i: jnp.where(ascends(strip), i, chunks + 1 - i)
    row_of = lambda i: pl.multiple_of(reach * (chunk_of(i) - 1), reach)
    inside = pl.ds(reach, depth)
    step_first = jnp.where(ascends(strip), -1, 1)
    strip_first, strip_last = strip + step_first, strip - step_first
    has_first = (strip_first >= 0) & (strip_first < 4)
    has_last = (strip_last >= 0) & (strip_last < 4)

    def row_of_part(part):
        before, after = starts[part], chunks - starts[part] - sizes[part]
        return pl.multiple_of(reach * jnp.where(ascends(strip), before, after), reach)

    def back_part(part):
        back_rows(row_of_part(part), reach * sizes[part], lzb_ref, s_ref, product_ref)

    def ratio_part(part, from_ref):
        row = row_of_part(part)
        ly_ref, lyb_ref = y_refs[2 * part], y_refs[2 * part + 1]

        ratio_planes(
            row, range(depth + 2 * pad), wide, data_ref, ly_ref, lyb_ref, xb_ref, from_ref, s_ref,
        )

    def places(part, body):
        pl.loop(1 + starts[part], 1 + starts[part] + sizes[part])(body)

    def swap(i):
        at = pl.ds(row_of(i), reach)
        return remote(product_ref.at[at], other_ref.at[at], (p_s, p_r), i, here.partner())

    to_block = k + 1 - 2 * c
    z_sends = (to_block >= 0) & (to_block < blocks)
    z_gets = (k - 1 + 2 * c >= 0) & (k - 1 + 2 * c < blocks)
    q_gets = (k + 1 - 2 * c >= 0) & (k + 1 - 2 * c < blocks)
    z_from = pl.multiple_of(reach + (1 - c) * (depth - reach), 8)
    z_to = pl.multiple_of(c * (reach + depth), 8)

    def along_z(i):
        at = pl.ds(reach + row_of(i), reach)
        return remote(
            est2_ref.at[at, pl.ds(z_from, reach)], est2_ref.at[at, pl.ds(z_to, reach)],
            (z_s, z_r), i, here.device(k=to_block),
        )

    def across(i):
        at = pl.ds(reach + row_of(i), reach)
        return remote(
            est2_ref.at[at, pl.ds(z_to, reach)], est2_ref.at[at, pl.ds(z_to, reach)],
            (q_s, q_r), i, here.partner(),
        )

    def to_strip(last, zone, index):
        place = chunks if last else 1
        return remote(
            est2_ref.at[pl.ds(reach + row_of(place), reach), zone],
            est2_ref.at[pl.ds(pl.multiple_of(
                jnp.where(ascends(strip) == bool(last), 0, reach + rows), reach), reach), zone],
            (y_s, y_r), index, here.of_strip(strip_last if last else strip_first),
        )

    def y_main(last):
        return to_strip(last, pl.ds(pl.multiple_of(reach + planes * c, 8), planes), last)

    def y_across(last):
        at = pl.ds(reach + row_of((chunks + 1) * last), reach)
        zone = pl.ds(pl.multiple_of(reach + planes * c, 8), planes)
        return remote(
            est2_ref.at[at, zone], est2_ref.at[at, zone], (q_s, q_r), chunks + 2 + last, here.partner(),
        )

    def y_corner(last):
        return to_strip(last, pl.ds(z_to, reach), 2 + last)

    unless(left)(lambda: zero(est2_ref, 0, reach, 0, depth + 2 * reach))
    unless(right)(lambda: zero(est2_ref, reach + rows, reach, 0, depth + 2 * reach))
    unless(below)(lambda: zero(est2_ref, 0, wide, 0, reach))
    unless(above)(lambda: zero(est2_ref, 0, wide, reach + depth, reach))

    late = 1 + starts[parts - 1]

    def first_update(part):
        ratio_part(part, t_ref)

        def make(i):
            swap(i).start()

        def use(i):
            swap(i).wait_recv()

            @pl.loop(0, reach, unroll=4)
            def _(r):
                row = row_of(i) + r
                factor = root(product_ref[row] * other_ref[row])
                est2_ref[reach + row, inside] = est_ref[reach + row, inside] * factor

            pl.when(z_sends)(along_z(i).start)
            pl.when((i == 1) & has_first)(y_main(0).start)
            pl.when((i == chunks) & has_last)(y_main(1).start)

        flip = lambda body: (lambda i: body(late + chunks - i)) if part == parts - 1 else body
        back_part(part)
        places(part, lambda i: flip(make)(i))
        places(part, lambda i: flip(use)(i))

    def arrive(i):
        @pl.when(z_gets)
        def _():
            along_z(i).wait_recv()
            pl.when((i == 1) & has_first)(y_corner(0).start)
            pl.when((i == chunks) & has_last)(y_corner(1).start)
            across(i).start()

    def arrive_side(last, there):
        @pl.when(there)
        def _():
            y_main(last).wait_recv()
            y_across(last).start()

            @pl.when(z_gets)
            def _():
                y_corner(last).wait_recv()
                across((chunks + 1) * last).start()

    def side_forward(last, there):
        pl.when(there)(y_across(last).wait_recv)
        forward((chunks + 1) * last)

    def forward(i):
        there = ((i > 0) | has_first) & ((i < chunks + 1) | has_last)
        pl.when(q_gets & there)(across(i).wait_recv)
        forward_rows(pl.multiple_of(reach * chunk_of(i), reach), reach, est2_ref, lz_ref, x_ref, t2_ref)

    half_rows = reach // 2

    def last_swap(i):
        at = pl.ds(row_of(i) + half_rows * (1 - c), half_rows)
        return remote(product_ref.at[at], other2_ref.at[at], (f_s, f_r), i, here.partner())

    new_stride = new_ref.shape[0] // depth
    new3 = new_ref.reshape(depth, new_stride, width_x)

    def my_half(i):
        return pl.ds(pl.multiple_of(row_of(i) + half_rows * c, 8), half_rows)

    def gather(i, kind):
        oa, ob = here.others()[kind]
        return remote(
            new3.at[pl.ds(planes * ob, planes), my_half(i)],
            all_ref.at[:, pl.ds(pl.multiple_of(rows * strip + my_half(i).start, 8), half_rows)],
            (g_s, g_r), 3 * i + kind, here.device(a=oa, b=ob),
        )

    def own(i):
        return remote(
            new3.at[pl.ds(planes * b, planes), my_half(i)],
            all_ref.at[:, pl.ds(pl.multiple_of(rows * strip + my_half(i).start, 8), half_rows)],
            (o_s, o_r), i, here.partner(),
        )

    def onward(i, kind):
        theirs = here.strip_of(*here.others()[kind])
        chunk = jnp.where(ascends(theirs), i - 1, chunks - i)
        at = pl.ds(pl.multiple_of(rows * theirs + reach * chunk + half_rows * c, 8), half_rows)
        return remote(all_ref.at[:, at], all_ref.at[:, at], (w_s, w_r), 3 * i + kind, here.partner())

    def last_update():

        def free(i):
            swap(i).wait_send()

        def make(i):
            last_swap(i).start()

        def use(i):
            last_swap(i).wait_recv()

            @pl.loop(0, half_rows, unroll=4)
            def _(r):
                row = row_of(i) + half_rows * c + r
                factor = root(product_ref[row] * other2_ref[row])
                new_ref[pl.ds(row, depth, stride=new_stride)] = est2_ref[reach + row, inside] * factor

            for kind in (2, 0, 1):
                gather(i, kind).start()
            own(i).start()

            @pl.loop(0, planes, unroll=8)
            def _(z):
                at = pl.ds(pl.multiple_of(rows * strip + my_half(i).start, 8), half_rows)
                all_ref[z, at] = new3[planes * b + z, my_half(i)]

        return free, make, use

    free, make, use = last_update()

    def make_part(part):
        ratio_part(part, t2_ref)
        places(part, free)
        back_part(part)
        places(part, make)

    for part in range(2, parts):
        edges_come(part)
    early = 1 + starts[parts - 2]
    for part in range(parts - 1):
        rest_comes(part)
        first_update(part)
    pl.loop(1, early)(arrive)
    pl.loop(1, early)(forward)
    rest_comes(parts - 1)
    first_update(parts - 1)
    pl.loop(early, late)(arrive)
    arrive_side(0, has_first)
    pl.loop(early, late)(forward)
    side_forward(0, has_first)
    for part in range(parts - 2):
        make_part(part)
    pl.loop(late, chunks + 1)(lambda i: arrive(late + chunks - i))
    for part in range(parts - 2):
        places(part, use)
    pl.loop(late, chunks + 1)(forward)
    make_part(parts - 2)
    arrive_side(1, has_last)
    places(parts - 2, use)
    side_forward(1, has_last)
    make_part(parts - 1)
    places(parts - 1, use)

    @pl.loop(1, chunks + 1)
    def _(i):
        for kind in range(3):
            gather(i, kind).wait_recv()
            onward(i, kind).start()

    @pl.loop(1, chunks + 1)
    def _(i):
        last_swap(i).wait_send()
        own(i).wait()
        for kind in range(3):
            gather(i, kind).wait_send()
            onward(i, kind).wait()
        pl.when(z_sends)(along_z(i).wait_send)

    for which in every_data:
        data_copy(*which).wait_send()
    for part in range(parts):
        for kind in range(4):
            pl.when(halo_goes(kind))(halo_copy(part, kind).wait_send)
    for last, there in enumerate((has_first, has_last)):
        pl.when(there)(y_main(last).wait_send)
        pl.when(there)(y_across(last).wait_send)
        pl.when(there & z_gets)(y_corner(last).wait_send)

    @pl.loop(0, chunks + 2)
    def _(i):
        there = ((i > 0) | has_first) & ((i < chunks + 1) | has_last)
        pl.when(z_gets & there)(across(i).wait_send)


def output_kernel(all_ref, out_ref):
    group = out_ref.shape[0]
    base = pl.program_id(0) * group
    for i in range(group):
        out_ref[i] = all_ref[base + i].T


def on_device(blocks, views_data, start, psf_table, psf_index):
    f32, bf16 = jnp.float32, jnp.bfloat16
    planes, width_x, width_y = start.shape
    reach = psf_table.shape[2] - 1
    pad = reach // 2
    rows = width_y // 4
    depth = 2 * planes
    wide, deep = rows + 2 * reach, depth + 2 * reach
    tall, outer = rows + 2 * pad, depth + 2 * pad
    chunks = rows // reach
    sizes = part_sizes(chunks)
    parts = len(sizes)
    y_matrices = []
    for size in sizes:
        own, mid, far = (reach * (size + more) for more in range(3))
        y_matrices.append(pltpu.VMEM((2, 2 * mid, 2 * far), bf16))
        y_matrices.append(pltpu.VMEM((2, 2 * own, 2 * mid), bf16))
    dma = lambda n: [pltpu.SemaphoreType.DMA((n,)), pltpu.SemaphoreType.DMA((n,))]

    by_row = jnp.transpose(psf_table, (1, 0, 2))
    gathered = pl.pallas_call(
        functools.partial(whole_kernel, blocks, rows),
        out_shape=jax.ShapeDtypeStruct((planes, width_y, width_x), f32),
        in_specs=[HBM, HBM, HBM, pl.BlockSpec(memory_space=pltpu.SMEM)],
        out_specs=VMEM,
        scratch_shapes=[
            pltpu.VMEM(start.shape, f32),
            pltpu.VMEM(by_row.shape, f32),
            pltpu.VMEM((planes, width_y + 2 * pad, width_x), f32),
            pltpu.VMEM((2, 8, 128), f32),
            pltpu.VMEM((wide, deep, width_x), f32),
            pltpu.VMEM((wide, deep, width_x), f32),
            pltpu.VMEM((2, outer, tall, width_x), f32),
            pltpu.VMEM((2, 2 * outer, 2 * deep), bf16),
            pltpu.VMEM((2, 2 * width_x, 2 * width_x), bf16),
            pltpu.VMEM((2, 2 * width_x, 2 * width_x), bf16),
            pltpu.VMEM((2, 2 * depth, 2 * outer), bf16),
            pltpu.VMEM((2 * wide * odd_stride(outer), width_x), f32),
            pltpu.VMEM((2 * wide * odd_stride(outer), width_x), f32),
            pltpu.VMEM((2, outer * odd_stride(rows), width_x), f32),
            pltpu.VMEM((rows, depth, width_x), f32),
            pltpu.VMEM((rows, depth, width_x), f32),
            pltpu.VMEM((rows, depth, width_x), f32),
            pltpu.VMEM((depth * odd_stride(rows), width_x), f32),
            *y_matrices,
            pltpu.SemaphoreType.DMA((2 * (planes // pad) + 1,)),
            *dma(1), *dma(6 + planes // pad), *dma(6 * parts), *dma(4 * parts),
            *dma(chunks + 1), *dma(4), *dma(chunks + 1), *dma(chunks + 4),
            *dma(chunks + 1), *dma(3 * chunks + 3), *dma(chunks + 1), *dma(3 * chunks + 3),
        ],
        compiler_params=pltpu.CompilerParams(
            collective_id=0, has_side_effects=True, vmem_limit_bytes=VMEM_LIMIT * MIB
        ),
    )(views_data[0], start, by_row, psf_index)
    return pl.pallas_call(
        output_kernel,
        grid=(planes // 8,),
        out_shape=jax.ShapeDtypeStruct(start.shape, f32),
        in_specs=[VMEM],
        out_specs=pl.BlockSpec((8, width_x, width_y), lambda i: (i, 0, 0)),
        compiler_params=pltpu.CompilerParams(vmem_limit_bytes=12 * MIB),
    )(gathered)


def solution(mesh):
    return jax.shard_map(
        functools.partial(on_device, mesh.shape["gz"] // 2),
        mesh=mesh,
        in_specs=(P("view", "gz", None, None), P("gz", None, None), P(), P("view")),
        out_specs=P("gz", None, None),
        check_vma=False,
    )
```
